32 devices in a mesh: gx: 16 (over z, y, core), gy: 2 (over x).
Axes of the slice: x: 2, y: 2, z: 4, core: 2. Of those that a mesh axis runs over, the one named last changes fastest.
Arguments:
- solution_vector: float32 [3, 256, 32, 128], P(None, 'gx', 'gy'), may hold values from -1 to 3, as said below
- insulator_marker: int32 [256, 32, 128], P('gx', 'gy'), may hold values 0 or 1
- electrode_marker: int32 [256, 32, 128], P('gx', 'gy'), may hold values 0 or 1
- impurity_zone_index: int32 [64, 8, 32], P('gx', 'gy'), may hold values from 0 to 3
- conductivity_category: int32 [64, 8, 32], P('gx', 'gy'), may hold values from 0 to 3
- warmth_rise: float32 [64, 8, 32], P('gx', 'gy'), may hold values from 0 to 2
Outputs:
- new_state: float32 [3, 256, 32, 128], P(None, 'gx', 'gy')
- new_temperature: float32 [64, 8, 32], P('gx', 'gy')
The draws below stay inside these ranges and needn't reach their ends.
Inputs may be any that keep to these rules, and one draw needn't show every extreme that they name: `solution_vector`: channel 0 is the potential; channels 1 and 2 are the electron and hole densities, which are positive.
All inputs are finite; a program needn't handle non-finite values. No bound on the sum of `insulator_marker` or of `electrode_marker` on one device may be relied on, other than what follows from the above.
Results may differ from the reference program's by a relative error of at most 0.0003.
Values sent between devices are 32-bit elements; how exact they have to be, the bound alone decides.
No kernel may reach another device: no remote copies, remote signals or barrier semaphores. Data moves between devices by JAX's collectives and lax.ppermute only.
A program may use at most 64 MiB of HBM per device.

```python
import math
import jax
import jax.numpy as jnp

LAYER_COUNT = 128
COARSEN_RATIO = 4
NEWTON = 3
SWEEPS = 3
COLUMN_COUNT = 256
ROW_COUNT = 32


def draw_solution_vector(key, part):
    key_pot = jax.random.fold_in(key, 11)
    species_label = jax.random.fold_in(key, 12)
    lattice_span = (COLUMN_COUNT, ROW_COUNT, LAYER_COUNT)
    voltage_field = jax.random.uniform(key_pot, lattice_span, jnp.float32, -0.5, 0.5)
    minimum_limit, maximum_limit = (0.5, 2.0)
    species_couple = jnp.exp(jax.random.uniform(species_label, (2,) + lattice_span, jnp.float32, math.log(minimum_limit), math.log(maximum_limit)))
    return jnp.concatenate([voltage_field[None], species_couple], 0)


def touch_ends(entries, key, smallest, largest):
    spot = [jax.random.randint(jax.random.fold_in(key, axis), (), 0, length) for axis, length in enumerate(entries.shape)]
    main_axis = entries.shape.index(max(entries.shape))
    neighbour = spot[:main_axis] + [(spot[main_axis] + 1) % entries.shape[main_axis]] + spot[main_axis + 1:]
    return entries.at[tuple(spot)].set(smallest).at[tuple(neighbour)].set(largest)


def block_scale(stream_key, extent, shards, smallest, largest):
    gain, own = 1.0, jax.random.fold_in(stream_key, 6)
    for axis_at, blocks in shards:
        heights = jnp.exp(jax.random.uniform(jax.random.fold_in(own, axis_at), (blocks,), jnp.float32, smallest / len(shards), largest / len(shards)))
        gain = gain * jnp.repeat(heights, extent[axis_at] // blocks).reshape([-1 if axis == axis_at else 1 for axis in range(len(extent))])
    return gain


def setup_inputs(seed: int = 0) -> dict:
    keys = jax.random.split(jax.random.key(seed), 7)
    solution_vector = draw_solution_vector(jax.random.fold_in(keys[6], 71), 0)
    insulator_marker = touch_ends((jax.random.randint(keys[1], (COLUMN_COUNT, ROW_COUNT, LAYER_COUNT), 0, 4) < 1).astype(jnp.int32), jax.random.fold_in(keys[1], 1), 0, 1)
    electrode_marker = touch_ends((jax.random.randint(keys[2], (COLUMN_COUNT, ROW_COUNT, LAYER_COUNT), 0, 16) < 1).astype(jnp.int32), jax.random.fold_in(keys[2], 1), 0, 1)
    impurity_zone_index = touch_ends(jax.random.randint(keys[3], (COLUMN_COUNT // COARSEN_RATIO, ROW_COUNT // COARSEN_RATIO, LAYER_COUNT // COARSEN_RATIO), 0, 4), jax.random.fold_in(keys[3], 1), 0, 3).astype(jnp.int32)
    conductivity_category = touch_ends(jax.random.randint(keys[4], (COLUMN_COUNT // COARSEN_RATIO, ROW_COUNT // COARSEN_RATIO, LAYER_COUNT // COARSEN_RATIO), 0, 4), jax.random.fold_in(keys[4], 1), 0, 3).astype(jnp.int32)
    warmth_rise = jnp.clip(2.0 * jax.random.uniform(keys[5], (COLUMN_COUNT // COARSEN_RATIO, ROW_COUNT // COARSEN_RATIO, LAYER_COUNT // COARSEN_RATIO), jnp.float32) ** block_scale(keys[5], (COLUMN_COUNT // COARSEN_RATIO, ROW_COUNT // COARSEN_RATIO, LAYER_COUNT // COARSEN_RATIO), ((0, 16), (1, 2)), -0.2, 0.2), 0.0, 2.0)
    return dict(solution_vector=solution_vector, insulator_marker=insulator_marker, electrode_marker=electrode_marker, impurity_zone_index=impurity_zone_index, conductivity_category=conductivity_category, warmth_rise=warmth_rise)


poisson_scale = 2.0
charge_scale = 4.0
clock_offset = 24.0
contact_bias = 0.25
heat_gain = 1.0
sink_rate = 0.3
speed_falloff = 0.5
dope_table = (-2.0, -0.5, 0.5, 2.0)
conduct_table = (0.5, 1.0, 2.0, 4.0)


def bernoulli(value):
    tiny = jnp.abs(value) < 1e-4
    safe = jnp.where(tiny, 1.0, jnp.expm1(value))
    return jnp.where(tiny, 1.0 - 0.5 * value, value / safe)


def bernoulli_slope(value):
    tiny = jnp.abs(value) < 0.05
    safe = jnp.where(tiny, 1.0, jnp.expm1(value))
    exact = (safe - value * jnp.exp(value)) / (safe * safe)
    series = -0.5 + value / 6.0 - value * value * value / 180.0
    return jnp.where(tiny, series, exact)


def neighbours(framed_array):
    return [framed_array[..., 2:, 1:-1, 1:-1], framed_array[..., :-2, 1:-1, 1:-1],
            framed_array[..., 1:-1, 2:, 1:-1], framed_array[..., 1:-1, :-2, 1:-1],
            framed_array[..., 1:-1, 1:-1, 2:], framed_array[..., 1:-1, 1:-1, :-2]]


def centre(framed_array):
    return framed_array[..., 1:-1, 1:-1, 1:-1]


def lookup(labels, table):
    result = jnp.zeros(labels.shape, jnp.float32)
    for level, amount in enumerate(table):
        result = result + jnp.where(labels == level, amount, 0.0)
    return result


def refine_warmth(coarse):
    lattice_span = coarse.shape
    spread = jnp.broadcast_to(coarse[:, None, :, None, :, None],
                              (lattice_span[0], COARSEN_RATIO, lattice_span[1], COARSEN_RATIO, lattice_span[2], COARSEN_RATIO))
    return spread.reshape(lattice_span[0] * COARSEN_RATIO, lattice_span[1] * COARSEN_RATIO, lattice_span[2] * COARSEN_RATIO)


def restrict(fine):
    lattice_span = fine.shape
    blocks = fine.reshape(lattice_span[0] // COARSEN_RATIO, COARSEN_RATIO, lattice_span[1] // COARSEN_RATIO, COARSEN_RATIO, lattice_span[2] // COARSEN_RATIO, COARSEN_RATIO)
    return jnp.mean(blocks, axis=(1, 3, 5))


def relax_weight(framed_array, warming_input, caloric_transfer):
    total = sum(neighbours(framed_array))
    return (warming_input + caloric_transfer * total) / (sink_rate + 6.0 * caloric_transfer)


def linearized_correction(framed_array, permittivity_framed, interior_frame_mask, impurity_profile, electrode_active, species_drift_speed):
    voltage_field = centre(framed_array[0])
    negative_density = centre(framed_array[1])
    positive_density = centre(framed_array[2])
    eps_here = centre(permittivity_framed)
    lap_sum = jnp.zeros_like(voltage_field)
    face_sum = jnp.zeros_like(voltage_field)
    negative_current = jnp.zeros_like(voltage_field)
    positive_current = jnp.zeros_like(voltage_field)
    negative_gradient = jnp.zeros_like(voltage_field)
    positive_gradient = jnp.zeros_like(voltage_field)
    backward_scharfetter = jnp.zeros_like(voltage_field)
    forward_scharfetter = jnp.zeros_like(voltage_field)
    ohmic_dissipation = jnp.zeros_like(voltage_field)
    parts = zip(neighbours(framed_array[0]), neighbours(framed_array[1]), neighbours(framed_array[2]),
                neighbours(permittivity_framed), neighbours(interior_frame_mask))
    for pot_near, elec_near, hole_near, eps_near, weight in parts:
        drop = pot_near - voltage_field
        plus = bernoulli(drop)
        minus = bernoulli(-drop)
        slope_plus = bernoulli_slope(drop)
        slope_minus = bernoulli_slope(-drop)
        face = weight * 0.5 * (eps_here + eps_near)
        lap_sum = lap_sum + face * drop
        face_sum = face_sum + face
        elec_flow = weight * (elec_near * plus - negative_density * minus)
        hole_flow = weight * (hole_near * minus - positive_density * plus)
        negative_current = negative_current + elec_flow
        positive_current = positive_current + hole_flow
        ohmic_dissipation = ohmic_dissipation + (elec_flow - hole_flow) * (elec_flow - hole_flow)
        negative_gradient = negative_gradient + weight * (-elec_near * slope_plus - negative_density * slope_minus)
        positive_gradient = positive_gradient + weight * (hole_near * slope_minus + positive_density * slope_plus)
        backward_scharfetter = backward_scharfetter + weight * minus
        forward_scharfetter = forward_scharfetter + weight * plus
    denom = negative_density + positive_density + 2.0
    annihilation_rate = (negative_density * positive_density - 1.0) / denom
    negative_generation = (positive_density + 1.0) * (positive_density + 1.0) / (denom * denom)
    positive_generation = (negative_density + 1.0) * (negative_density + 1.0) / (denom * denom)
    res_psi = poisson_scale * lap_sum + charge_scale * (positive_density - negative_density + impurity_profile)
    negative_mismatch = species_drift_speed * negative_current - annihilation_rate
    positive_mismatch = species_drift_speed * positive_current - annihilation_rate
    blank_array = jnp.zeros_like(voltage_field)
    unit_array = jnp.ones_like(voltage_field)
    res_psi = jnp.where(electrode_active, voltage_field - contact_bias * impurity_profile, res_psi)
    negative_mismatch = jnp.where(electrode_active, negative_density - 1.0, negative_mismatch)
    positive_mismatch = jnp.where(electrode_active, positive_density - 1.0, positive_mismatch)
    mat_aa = jnp.where(electrode_active, unit_array, -poisson_scale * face_sum)
    mat_ab = jnp.where(electrode_active, blank_array, -charge_scale * unit_array)
    mat_ac = jnp.where(electrode_active, blank_array, charge_scale * unit_array)
    jacobian_entry_second_first = jnp.where(electrode_active, blank_array, species_drift_speed * negative_gradient)
    jacobian_entry_second_second = jnp.where(electrode_active, unit_array, -species_drift_speed * backward_scharfetter - negative_generation - clock_offset)
    mat_bc = jnp.where(electrode_active, blank_array, -positive_generation)
    jacobian_entry_third_first = jnp.where(electrode_active, blank_array, species_drift_speed * positive_gradient)
    mat_cb = jnp.where(electrode_active, blank_array, -negative_generation)
    jacobian_entry_third_third = jnp.where(electrode_active, unit_array, -species_drift_speed * forward_scharfetter - positive_generation - clock_offset)
    cof_aa = jacobian_entry_second_second * jacobian_entry_third_third - mat_bc * mat_cb
    cof_ab = mat_bc * jacobian_entry_third_first - jacobian_entry_second_first * jacobian_entry_third_third
    cof_ac = jacobian_entry_second_first * mat_cb - jacobian_entry_second_second * jacobian_entry_third_first
    determ = mat_aa * cof_aa + mat_ab * cof_ab + mat_ac * cof_ac
    step_psi = (cof_aa * res_psi + (mat_ac * mat_cb - mat_ab * jacobian_entry_third_third) * negative_mismatch
                + (mat_ab * mat_bc - mat_ac * jacobian_entry_second_second) * positive_mismatch) / determ
    step_n = (cof_ab * res_psi + (mat_aa * jacobian_entry_third_third - mat_ac * jacobian_entry_third_first) * negative_mismatch
              + (mat_ac * jacobian_entry_second_first - mat_aa * mat_bc) * positive_mismatch) / determ
    step_p = (cof_ac * res_psi + (mat_ab * jacobian_entry_third_first - mat_aa * mat_cb) * negative_mismatch
              + (mat_aa * jacobian_entry_second_second - mat_ab * jacobian_entry_second_first) * positive_mismatch) / determ
    new_pot = voltage_field - step_psi
    new_elec = negative_density * jnp.exp(-step_n / negative_density)
    new_hole = positive_density * jnp.exp(-step_p / positive_density)
    warming_field = 0.5 * species_drift_speed * ohmic_dissipation / (negative_density + positive_density)
    return jnp.stack([new_pot, new_elec, new_hole], 0), warming_field


def reference(solution_vector, insulator_marker, electrode_marker, impurity_zone_index, conductivity_category, warmth_rise):
    eps = jnp.where(insulator_marker == 1, 0.4, 1.0).astype(solution_vector.dtype)
    permittivity_framed = jnp.pad(eps, 1)
    interior_frame_mask = jnp.pad(jnp.ones_like(eps), 1)
    impurity_profile = refine_warmth(lookup(impurity_zone_index, dope_table))
    caloric_transfer = lookup(conductivity_category, conduct_table)
    electrode_active = electrode_marker == 1
    for newton_step in range(NEWTON):
        species_drift_speed = 1.0 / (1.0 + speed_falloff * refine_warmth(warmth_rise))
        framed_array = jnp.pad(solution_vector, ((0, 0), (1, 1), (1, 1), (1, 1)))
        solution_vector, warming_field = linearized_correction(framed_array, permittivity_framed, interior_frame_mask, impurity_profile, electrode_active, species_drift_speed)
        warming_input = heat_gain * restrict(warming_field)
        for sweep in range(SWEEPS):
            warmth_rise = relax_weight(jnp.pad(warmth_rise, 1), warming_input, caloric_transfer)
    return solution_vector, warmth_rise
```

```python
import jax
import jax.numpy as jnp
from jax import lax
from jax.experimental import pallas as pl
from jax.experimental.pallas import tpu as pltpu
from jax.sharding import PartitionSpec as P

R = 4
NEWTON = 3
SWEEPS = 3

POISSON = 2.0
CHARGE = 4.0
SHIFT = 24.0
BIAS = 0.25
GAIN = 1.0
SINK = 0.3
DROP = 0.5
DOPING = (-2.0, -0.5, 0.5, 2.0)
CONDUCT = (0.5, 1.0, 2.0, 4.0)

F32 = jnp.float32


def phases(count):
    out = []
    for start in (0, 1):
        pairs = []
        for i in range(start, count - 1, 2):
            pairs += [(i, i + 1), (i + 1, i)]
        if pairs:
            out.append(pairs)
    return out


def both(pairs_x, pairs_y, count_y):
    return [(i * count_y + j, k * count_y + m) for i, k in pairs_x for j, m in pairs_y]


def lookup(labels, table):
    value = jnp.full(labels.shape, table[0], F32)
    for level in range(1, len(table)):
        value = jnp.where(labels == level, table[level], value)
    return value


def face(here, there, weight=None):
    psi_i, n_i, p_i, e_i = here
    psi_j, n_j, p_j, e_j = there
    d = psi_j - psi_i
    small = jnp.abs(d) < 0.25
    r = 1.0 / jnp.where(small, 1.0, jnp.exp(d) - 1.0)
    q = d * d
    b = jnp.where(
        small, (1.0 - 0.5 * d) + q * (1 / 12 - q * (1 / 720 - q * (1 / 30240))), d * r
    )
    bm = b + d
    s = jnp.where(small, -0.5 + d * (1 / 6 - q * (1 / 180 - q * (1 / 5040))), r * (1.0 - bm))
    e = 0.5 * (e_i + e_j)
    if weight is None:
        gn = n_i + (n_i - n_j) * s
        gp = (p_i - p_j) * s - p_j
    else:
        b = b * weight
        bm = b + d * weight
        s = s * weight
        e = e * weight
        gn = n_i * weight + (n_i - n_j) * s
        gp = (p_i - p_j) * s - p_j * weight
    fe = n_j * b - n_i * bm
    fh = p_j * bm - p_i * b
    j = fe - fh
    return e * d, e, fe, fh, gn, gp, b, bm, j * j


def add_here(acc, f):
    lap, es, fe, fh, gn, gp, b, bm, h = f
    return [x + y for x, y in zip(acc, (lap, es, fe, fh, gn, gp, b, bm, h))]


def add_there(acc, f):
    lap, es, fe, fh, gn, gp, b, bm, h = f
    return [
        acc[0] - lap, acc[1] + es, acc[2] - fe, acc[3] - fh,
        acc[4] + gn, acc[5] + gp, acc[6] + bm, acc[7] + b, acc[8] + h,
    ]


def solve(here, acc, contact, dop, mob):
    psi, n, p, _ = here
    lap, es, fe, fh, gn, gp, fwd, bwd, h = acc
    total = n + p
    rden = 1.0 / (total + 2.0)
    rec = (n * p - 1.0) * rden
    rn = (p + 1.0) * rden
    rn = rn * rn
    rp = (n + 1.0) * rden
    rp = rp * rp
    r0 = POISSON * lap + CHARGE * (p - n + dop)
    r1 = mob * fe - rec
    r2 = mob * fh - rec
    a = -POISSON * es
    b1 = mob * gn
    b2 = -mob * bwd - rn - SHIFT
    g1 = mob * gp
    g3 = -mob * fwd - rp - SHIFT
    caa = b2 * g3 - rp * rn
    cab = -(rp * g1 + b1 * g3)
    cac = -(b1 * rn + b2 * g1)
    rdet = 1.0 / (a * caa + CHARGE * (cac - cab))
    cb1 = CHARGE * b1
    cg1 = CHARGE * g1
    s0 = (caa * r0 + CHARGE * ((g3 - rn) * r1 + (rp - b2) * r2)) * rdet
    s1 = (cab * r0 + (a * g3 - cg1) * r1 + (cb1 + a * rp) * r2) * rdet
    s2 = (cac * r0 + (a * rn - cg1) * r1 + (a * b2 + cb1) * r2) * rdet
    s0 = jnp.where(contact, psi - BIAS * dop, s0)
    s1 = jnp.where(contact, n - 1.0, s1)
    s2 = jnp.where(contact, p - 1.0, s2)
    heat = h / total
    return psi - s0, n * jnp.exp(-s1 / n), p * jnp.exp(-s2 / p), heat


def iota(shape, axis):
    return lax.broadcasted_iota(jnp.int32, shape, axis)


def spread_rows(ref, first, count):
    lanes = ref.shape[-1]
    group = iota((count * R, lanes), 0) // R
    out = jnp.broadcast_to(ref[first : first + 1, :], (count * R, lanes))
    for j in range(1, count):
        out = jnp.where(group == j, ref[first + j : first + j + 1, :], out)
    return out


def make(nx, ny, nz, gx, gy):
    cx, cy = nx // R, ny // R
    cells = cx * cy
    W = SWEEPS
    px, py = phases(gx), phases(gy)
    ux, uy = len(px), len(py)
    ex, ey = cx + 2 * W, -(-(cy + 2 * W) // 8) * 8
    params = pltpu.CompilerParams(vmem_limit_bytes=16 * 1024 * 1024)
    smem = pl.BlockSpec(memory_space=pltpu.SMEM)
    vmem = pl.BlockSpec(memory_space=pltpu.VMEM)

    def call(kernel, outs, scratch, args, cost):
        return pl.pallas_call(
            kernel,
            out_shape=[jax.ShapeDtypeStruct(s, F32) for s in outs],
            in_specs=[smem] + [vmem] * (len(args) - 1),
            out_specs=[vmem] * len(outs),
            scratch_shapes=scratch,
            compiler_params=params,
            cost_estimate=pl.CostEstimate(
                flops=cost, bytes_accessed=0, transcendentals=0
            ),
        )(*args)

    def pick(odd, which, values):
        low_phase_even = 1 - which
        get = lambda k: values[k] if k < len(values) else jnp.zeros_like(values[0])
        return jnp.where(odd, get(1 - low_phase_even), get(low_phase_even))

    def put_sends(info, fields, sends):
        odd_x, odd_y = info[4] > 0.5, info[5] > 0.5
        for f, ref in enumerate(fields):
            low, high = ref[0:ny, :], ref[(nx - 1) * ny : nx * ny, :]
            rows = slice(f * ny, (f + 1) * ny)
            sends[0][rows, :] = jnp.where(odd_x, low, high)
            if ux > 1:
                sends[1][rows, :] = jnp.where(odd_x, high, low)
            low = ref[pl.ds(0, nx, stride=ny), :]
            high = ref[pl.ds(ny - 1, nx, stride=ny), :]
            rows = slice(f * nx, (f + 1) * nx)
            sends[ux][rows, :] = jnp.where(odd_y, low, high)
            if uy > 1:
                sends[ux + 1][rows, :] = jnp.where(odd_y, high, low)

    def pack_kernel(info, state, ins, zone, cat, warm, *rest):
        sends, (dop, cond, temp), eps = rest[: ux + uy], rest[ux + uy : ux + uy + 3], rest[-1]
        eps[...] = jnp.where(ins[...] == 1, 0.4, 1.0)
        put_sends(info, [state.at[0], state.at[1], state.at[2], eps], sends)
        coarse = nz // R
        pickz = (iota((coarse, nz), 1) // R == iota((coarse, nz), 0)).astype(F32)

        def widen(x):
            return jnp.dot(x, pickz, precision=lax.Precision.HIGHEST, preferred_element_type=F32)

        dop[...] = widen(lookup(zone[...], DOPING))
        cond[...] = widen(lookup(cat[...], CONDUCT))
        temp[...] = widen(warm[...])

    def sweeps(info, own, tiles_x, tiles_y, tiles_xy, base, ext):
        odd_x, odd_y = info[4] > 0.5, info[5] > 0.5
        ext[...] = jnp.zeros_like(ext)

        def grab(refs, f, off):
            return [r[off + f * cells : off + (f + 1) * cells, :] for r in refs]

        def place(f, sx, sy, tile):
            xs = {-1: range(cx - W, cx), 0: range(cx), 1: range(W)}[sx]
            ys = {-1: (cy - W, cy, 0), 0: (0, cy, W), 1: (0, W, W + cy)}[sy]
            at = {-1: 0, 0: W, 1: W + cx}[sx]
            for k, x in enumerate(xs):
                ext[f * ex + at + k, ys[2] : ys[2] + ys[1] - ys[0], :] = tile[
                    x * cy + ys[0] : x * cy + ys[1], :
                ]

        for f in range(3):
            place(f, 0, 0, own[f])
            for sx in (-1, 1):
                place(f, sx, 0, pick(odd_x, (sx + 1) // 2, grab(tiles_x, f, base[0])))
            for sy in (-1, 1):
                place(f, 0, sy, pick(odd_y, (sy + 1) // 2, grab(tiles_y, f, base[1])))
            for sx in (-1, 1):
                cols = []
                for row in tiles_xy:
                    cols.append(grab(row, f, 0))
                for sy in (-1, 1):
                    along = [pick(odd_y, (sy + 1) // 2, c) for c in cols]
                    place(f, sx, sy, pick(odd_x, (sx + 1) // 2, along))
        lane = iota((ey, nz), 1)
        has_low, has_high = lane >= R, lane < nz - R
        src = [ext[x] for x in range(ex)]
        tem = [ext[ex + x] for x in range(ex)]
        con = [ext[2 * ex + x] for x in range(ex)]
        inv = [1.0 / (SINK + 6.0 * c) for c in con]
        for s in range(1, W + 1):
            new = list(tem)
            for x in range(s, ex - s):
                t = tem[x]
                total = tem[x - 1] + tem[x + 1]
                total = total + (pltpu.roll(t, 1, 0) + pltpu.roll(t, ey - 1, 0))
                total = total + jnp.where(has_low, pltpu.roll(t, R, 1), 0.0)
                total = total + jnp.where(has_high, pltpu.roll(t, nz - R, 1), 0.0)
                new[x] = (src[x] + con[x] * total) * inv[x]
            tem = new
        return [tem[W + x][W : W + cy, :] for x in range(cx)]

    def newton_kernel(k):
        first, last = k == 0, k == NEWTON - 1

        def kernel(info, state, ins, ele, dop, cond, *rest):
            rest = list(rest)
            take = lambda c: [rest.pop(0) for _ in range(c)]
            got0 = take(ux + uy)
            if first:
                (temp_in,) = take(1)
                got, diag = got0, None
            else:
                got = take(ux + uy)
                diag = [take(uy) for _ in range(ux)]
                (tile,) = take(1)
            (out,) = take(1)
            sends = take(0 if last else ux + uy)
            (tile_out,) = take(1)
            halo, lowf, temp, heat, ext, mobs = take(6)
            odd_x, odd_y = info[4] > 0.5, info[5] > 0.5

            if first:
                temp[...] = temp_in[...]
            else:
                own = [tile[f * cells : (f + 1) * cells, :] for f in range(3)]
                rows = sweeps(info, own, got[:ux], got[ux:], diag, (3 * ny, 3 * nx), ext)
                for x in range(cx):
                    temp[x * cy : (x + 1) * cy, :] = rows[x]
            mobs[...] = 1.0 / (1.0 + DROP * temp[...])

            def side(axis, which, f):
                src = got0 if f == 3 else got
                if axis == 0:
                    return pick(odd_x, which, [r[f * ny : (f + 1) * ny, :] for r in src[:ux]])
                return pick(odd_y, which, [r[f * nx : (f + 1) * nx, :] for r in src[ux:]])

            epsof = lambda marks: jnp.where(marks == 1, 0.4, 1.0)
            row0 = [state[f, pl.ds(0, nx, stride=ny), :] for f in range(3)]
            row0.append(epsof(ins[pl.ds(0, nx, stride=ny), :]))
            below = [side(1, 0, f) for f in range(4)]
            for q, v in enumerate(face(below, row0, info[2])):
                lowf[q] = v
            for f in range(4):
                halo[f] = side(1, 1, f)

            zlane = iota((ny, nz), 1)
            wz = jnp.where(zlane < nz - 1, 1.0, 0.0)
            yrow = iota((ny, nz), 0)
            top = yrow == ny - 1
            bottom = yrow == 0
            wy = jnp.where(top, info[3], 1.0)

            def plane(x):
                rows = slice(x * ny, (x + 1) * ny)
                return [state[0, rows, :], state[1, rows, :], state[2, rows, :], epsof(ins[rows, :])]

            zero = jnp.zeros((ny, nz), F32)
            here = plane(0)
            acc = add_there(
                [zero] * 9, face([side(0, 0, f) for f in range(4)], here, info[0])
            )
            hsum = None
            for x in range(nx):
                if x % R == 0:
                    mob = spread_rows(mobs, (x // R) * cy, cy)
                    dopx = spread_rows(dop, (x // R) * cy, cy)
                if x + 1 < nx:
                    nxt = plane(x + 1)
                    f = face(here, nxt)
                else:
                    nxt = [side(0, 1, f) for f in range(4)]
                    f = face(here, nxt, info[1])
                acc = add_here(acc, f)
                later = add_there([zero] * 9, f)
                f = face(here, [pltpu.roll(v, nz - 1, 1) for v in here], wz)
                acc = add_here(acc, f)
                acc = add_there(acc, [pltpu.roll(v, 1, 1) for v in f])
                up = [
                    jnp.where(top, halo[q, x : x + 1, :], pltpu.roll(v, ny - 1, 0))
                    for q, v in enumerate(here)
                ]
                f = face(here, up, wy)
                acc = add_here(acc, f)
                f = [
                    jnp.where(bottom, lowf[q, x : x + 1, :], pltpu.roll(v, 1, 0))
                    for q, v in enumerate(f)
                ]
                acc = add_there(acc, f)
                contact = ele[slice(x * ny, (x + 1) * ny), :] == 1
                psi, n, p, h = solve(here, acc, contact, dopx, mob)
                rows = slice(x * ny, (x + 1) * ny)
                out[0, rows, :] = psi
                out[1, rows, :] = n
                out[2, rows, :] = p
                hsum = h if x % R == 0 else hsum + h
                if x % R == R - 1:
                    xc = x // R
                    heat[xc * ny : (xc + 1) * ny, :] = hsum
                here, acc = nxt, later

            v = heat[pl.ds(0, cells, stride=R), :]
            for j in range(1, R):
                v = v + heat[pl.ds(j, cells, stride=R), :]
            lane = iota((cells, nz), 1)
            step = 1
            while step < R:
                v = v + jnp.where(
                    lane % (2 * step) < step, pltpu.roll(v, nz - step, 1), pltpu.roll(v, step, 1)
                )
                step *= 2
            source = (GAIN * 0.5 / R**3) * mobs[...] * v
            tile_out[0:cells, :] = source
            tile_out[cells : 2 * cells, :] = temp[...]
            tile_out[2 * cells : 3 * cells, :] = cond[...]
            if not last:
                put_sends(info, [out.at[f] for f in range(3)], sends)
                for k2, s in enumerate(sends):
                    base = 3 * ny if k2 < ux else 3 * nx
                    s[base : base + 3 * cells, :] = tile_out[...]

        return kernel

    def final_kernel(info, *rest):
        rest = list(rest)
        take = lambda c: [rest.pop(0) for _ in range(c)]
        got = take(ux + uy)
        diag = [take(uy) for _ in range(ux)]
        tile, out, ext = take(3)
        own = [tile[f * cells : (f + 1) * cells, :] for f in range(3)]
        rows = sweeps(info, own, got[:ux], got[ux:], diag, (0, 0), ext)
        coarse = nz // R
        sel = (iota((nz, coarse), 0) == R * iota((nz, coarse), 1)).astype(F32)
        for x in range(cx):
            out[x * cy : (x + 1) * cy, :] = jnp.dot(
                rows[x], sel, precision=lax.Precision.HIGHEST, preferred_element_type=F32
            )

    def exchange(sends, tile=None):
        got = []
        for k, pairs in enumerate(px):
            got.append(lax.ppermute(sends[k], "gx", pairs))
        for k, pairs in enumerate(py):
            got.append(lax.ppermute(sends[ux + k], "gy", pairs))
        diag = []
        if tile is not None:
            for a in px:
                for b in py:
                    diag.append(lax.ppermute(tile, ("gx", "gy"), both(a, b, gy)))
        return got, diag

    def per_device(sol, ins, ele, zone, cat, warm):
        state = sol.reshape(3, nx * ny, nz)
        ins = ins.reshape(nx * ny, nz)
        ele = ele.reshape(nx * ny, nz)
        coarse = nz // R
        ix, iy = lax.axis_index("gx"), lax.axis_index("gy")
        info = jnp.stack(
            [ix > 0, ix < gx - 1, iy > 0, iy < gy - 1, ix % 2 == 1, iy % 2 == 1]
        ).astype(F32)
        rows_of = lambda extra: [(extra[0], nz)] * ux + [(extra[1], nz)] * uy
        node = nx * ny * nz
        res = call(
            pack_kernel,
            rows_of((4 * ny, 4 * nx)) + [(cells, nz)] * 3,
            [pltpu.VMEM((nx * ny, nz), F32)],
            [info, state, ins, zone.reshape(cells, coarse), cat.reshape(cells, coarse),
             warm.reshape(cells, coarse)],
            node,
        )
        sends, (dop, cond, temp) = res[: ux + uy], res[ux + uy :]
        got0, _ = exchange(sends)
        got, diag, tile = got0, [], None
        for k in range(NEWTON):
            last = k == NEWTON - 1
            args = [info, state, ins, ele, dop, cond] + got0
            args += [temp] if k == 0 else got + diag + [tile]
            outs = [(3, nx * ny, nz)]
            if not last:
                outs += rows_of((3 * ny + 3 * cells, 3 * nx + 3 * cells))
            outs += [(3 * cells, nz)]
            scratch = [
                pltpu.VMEM((4, nx, nz), F32),
                pltpu.VMEM((9, nx, nz), F32),
                pltpu.VMEM((cells, nz), F32),
                pltpu.VMEM((cx * ny, nz), F32),
                pltpu.VMEM((3 * ex, ey, nz), F32),
                pltpu.VMEM((cells, nz), F32),
            ]
            res = call(newton_kernel(k), outs, scratch, args, 300 * node)
            state, tile = res[0], res[-1]
            sends = [tile] * (ux + uy) if last else res[1:-1]
            got, diag = exchange(sends, tile)
        (warm,) = call(
            final_kernel,
            [(cells, coarse)],
            [pltpu.VMEM((3 * ex, ey, nz), F32)],
            [info] + got + diag + [tile],
            node,
        )
        return state.reshape(3, nx, ny, nz), warm.reshape(cx, cy, coarse)

    return per_device


def solution(mesh):
    placed = (
        P(None, "gx", "gy", None),
        P("gx", "gy", None),
        P("gx", "gy", None),
        P("gx", "gy", None),
        P("gx", "gy", None),
        P("gx", "gy", None),
    )
    gx, gy = mesh.shape["gx"], mesh.shape["gy"]

    def body(sol, *rest):
        _, nx, ny, nz = sol.shape
        return make(nx, ny, nz, gx, gy)(sol, *rest)

    return jax.shard_map(
        body,
        mesh=mesh,
        in_specs=placed,
        out_specs=(P(None, "gx", "gy", None), P("gx", "gy", None)),
        check_vma=False,
    )
```

```python
import jax
import jax.numpy as jnp
from jax import lax
from jax.experimental import pallas as pl
from jax.experimental.pallas import tpu as pltpu
from jax.sharding import PartitionSpec as P

R = 4
NEWTON = 3
SWEEPS = 3

POISSON = 2.0
CHARGE = 4.0
SHIFT = 24.0
BIAS = 0.25
GAIN = 1.0
SINK = 0.3
DROP = 0.5
DOPING = (-2.0, -0.5, 0.5, 2.0)
CONDUCT = (0.5, 1.0, 2.0, 4.0)

F32 = jnp.float32


def phases(count):
    out = []
    for start in (0, 1):
        pairs = []
        for i in range(start, count - 1, 2):
            pairs += [(i, i + 1), (i + 1, i)]
        if pairs:
            out.append(pairs)
    return out


def both(pairs_x, pairs_y, count_y):
    return [(i * count_y + j, k * count_y + m) for i, k in pairs_x for j, m in pairs_y]


def lookup(labels, table):
    value = jnp.full(labels.shape, table[0], F32)
    for level in range(1, len(table)):
        value = jnp.where(labels == level, table[level], value)
    return value


def face(here, there, weight=None):
    psi_i, n_i, p_i, e_i = here
    psi_j, n_j, p_j, e_j = there
    d = psi_j - psi_i
    small = jnp.abs(d) < 0.25
    r = 1.0 / jnp.where(small, 1.0, jnp.exp(d) - 1.0)
    q = d * d
    b = jnp.where(
        small, (1.0 - 0.5 * d) + q * (1 / 12 - q * (1 / 720 - q * (1 / 30240))), d * r
    )
    bm = b + d
    s = jnp.where(small, -0.5 + d * (1 / 6 - q * (1 / 180 - q * (1 / 5040))), r * (1.0 - bm))
    e = 0.5 * (e_i + e_j)
    if weight is None:
        gn = n_i + (n_i - n_j) * s
        gp = (p_i - p_j) * s - p_j
    else:
        b = b * weight
        bm = b + d * weight
        s = s * weight
        e = e * weight
        gn = n_i * weight + (n_i - n_j) * s
        gp = (p_i - p_j) * s - p_j * weight
    fe = n_j * b - n_i * bm
    fh = p_j * bm - p_i * b
    j = fe - fh
    return e * d, e, fe, fh, gn, gp, b, bm, j * j


def add_here(acc, f):
    lap, es, fe, fh, gn, gp, b, bm, h = f
    return [x + y for x, y in zip(acc, (lap, es, fe, fh, gn, gp, b, bm, h))]


def add_there(acc, f):
    lap, es, fe, fh, gn, gp, b, bm, h = f
    return [
        acc[0] - lap, acc[1] + es, acc[2] - fe, acc[3] - fh,
        acc[4] + gn, acc[5] + gp, acc[6] + bm, acc[7] + b, acc[8] + h,
    ]


def solve(here, acc, contact, dop, mob):
    psi, n, p, _ = here
    lap, es, fe, fh, gn, gp, fwd, bwd, h = acc
    total = n + p
    rden = 1.0 / (total + 2.0)
    rec = (n * p - 1.0) * rden
    rn = (p + 1.0) * rden
    rn = rn * rn
    rp = (n + 1.0) * rden
    rp = rp * rp
    r0 = POISSON * lap + CHARGE * (p - n + dop)
    r1 = mob * fe - rec
    r2 = mob * fh - rec
    a = -POISSON * es
    b1 = mob * gn
    b2 = -mob * bwd - rn - SHIFT
    g1 = mob * gp
    g3 = -mob * fwd - rp - SHIFT
    caa = b2 * g3 - rp * rn
    cab = -(rp * g1 + b1 * g3)
    cac = -(b1 * rn + b2 * g1)
    rdet = 1.0 / (a * caa + CHARGE * (cac - cab))
    cb1 = CHARGE * b1
    cg1 = CHARGE * g1
    s0 = (caa * r0 + CHARGE * ((g3 - rn) * r1 + (rp - b2) * r2)) * rdet
    s1 = (cab * r0 + (a * g3 - cg1) * r1 + (cb1 + a * rp) * r2) * rdet
    s2 = (cac * r0 + (a * rn - cg1) * r1 + (a * b2 + cb1) * r2) * rdet
    s0 = jnp.where(contact, psi - BIAS * dop, s0)
    s1 = jnp.where(contact, n - 1.0, s1)
    s2 = jnp.where(contact, p - 1.0, s2)
    heat = None if h is None else h / total
    return psi - s0, n * jnp.exp(-s1 / n), p * jnp.exp(-s2 / p), heat


def iota(shape, axis):
    return lax.broadcasted_iota(jnp.int32, shape, axis)


def spread_rows(ref, first, count):
    lanes = ref.shape[-1]
    group = iota((count * R, lanes), 0) // R
    out = jnp.broadcast_to(ref[first : first + 1, :], (count * R, lanes))
    for j in range(1, count):
        out = jnp.where(group == j, ref[first + j : first + j + 1, :], out)
    return out


def make(nx, ny, nz, gx, gy):
    cx, cy = nx // R, ny // R
    cells = cx * cy
    W = SWEEPS
    px, py = phases(gx), phases(gy)
    ux, uy = len(px), len(py)
    ex, ey = cx + 2 * W, -(-(cy + 2 * W) // 8) * 8
    nodes = nx * ny
    params = pltpu.CompilerParams(vmem_limit_bytes=16 * 1024 * 1024)
    smem = pl.BlockSpec(memory_space=pltpu.SMEM)
    vmem = pl.BlockSpec(memory_space=pltpu.VMEM)
    hbm = pl.BlockSpec(memory_space=pl.ANY)

    def call(kernel, outs, scratch, args, cost, specs=None):
        return list(pl.pallas_call(
            kernel,
            out_shape=[jax.ShapeDtypeStruct(s, F32) for s in outs],
            in_specs=specs or [smem] + [vmem] * (len(args) - 1),
            out_specs=[vmem] * len(outs),
            scratch_shapes=scratch,
            compiler_params=params,
            cost_estimate=pl.CostEstimate(flops=cost, bytes_accessed=0, transcendentals=0),
        )(*args))

    def pick(odd, which, values):
        get = lambda k: values[k] if k < len(values) else jnp.zeros_like(values[0])
        return jnp.where(odd, get(which), get(1 - which))

    def put_x(info, fields, sends):
        odd = info[4] > 0.5
        for f, ref in enumerate(fields):
            low, high = ref[0:ny, :], ref[(nx - 1) * ny : nodes, :]
            for k, send in enumerate(sends):
                first, second = (low, high) if k == 0 else (high, low)
                send[f * ny : (f + 1) * ny, :] = jnp.where(odd, first, second)

    def put_y(info, fields, sends):
        odd = info[5] > 0.5
        for f, ref in enumerate(fields):
            low = ref[pl.ds(0, nx, stride=ny), :]
            high = ref[pl.ds(ny - 1, nx, stride=ny), :]
            for k, send in enumerate(sends):
                first, second = (low, high) if k == 0 else (high, low)
                send[f * nx : (f + 1) * nx, :] = jnp.where(odd, first, second)

    def epsof(marks):
        return jnp.where(marks == 1, 0.4, 1.0)

    def turn(f):
        lap, es, fe, fh, gn, gp, b, bm, h = f
        return [-lap, es, -fe, -fh, gn, gp, bm, b, h]

    def whole(accs, rim_x, rim_y, x, qs):
        row = iota((8, nz), 0)
        out = []
        for q in qs:
            a = accs[q][x * ny : (x + 1) * ny, :]
            if x == 0:
                a = a + rim_x[q]
            if x == nx - 1:
                a = a + rim_x[9 + q]
            parts = [a[r : r + 8] for r in range(0, ny, 8)]
            parts[0] = parts[0] + jnp.where(row == 0, rim_y[q, x : x + 1, :], 0.0)
            parts[-1] = parts[-1] + jnp.where(row == 7, rim_y[9 + q, x : x + 1, :], 0.0)
            out.append(jnp.concatenate(parts, 0) if len(parts) > 1 else parts[0])
        return out

    def pack_kernel(info, state_h, ins_h, zone, cat, warm, *rest):
        sends, (dop, cond, temp) = rest[: ux + uy], rest[ux + uy : ux + uy + 3]
        state, eps, marks, sems = rest[ux + uy + 3 :]
        copies = [
            pltpu.make_async_copy(state_h, state, sems.at[0]),
            pltpu.make_async_copy(ins_h, marks, sems.at[1]),
        ]
        for c in copies:
            c.start()
        coarse = nz // R
        pickz = (iota((coarse, nz), 1) // R == iota((coarse, nz), 0)).astype(F32)

        def widen(x):
            return jnp.dot(x, pickz, precision=lax.Precision.HIGHEST, preferred_element_type=F32)

        dop[...] = widen(lookup(zone[...], DOPING))
        cond[...] = widen(lookup(cat[...], CONDUCT))
        temp[...] = widen(warm[...])
        for c in copies:
            c.wait()
        eps[...] = epsof(marks[...])
        fields = [state.at[0], state.at[1], state.at[2], eps]
        put_x(info, fields, sends[:ux])
        put_y(info, fields, sends[ux:])

    def inner_kernel(info, state, ins, *accs):
        zlane = iota((ny, nz), 1)
        wz = jnp.where(zlane < nz - 1, 1.0, 0.0)
        wy = jnp.where(iota((ny, nz), 0) < ny - 1, 1.0, 0.0)

        def plane(x):
            rows = slice(x * ny, (x + 1) * ny)
            return [state[0, rows, :], state[1, rows, :], state[2, rows, :], epsof(ins[rows, :])]

        here = plane(0)
        acc = None
        for x in range(nx):
            f = face(here, [pltpu.roll(v, nz - 1, 1) for v in here], wz)
            acc = list(f) if acc is None else add_here(acc, f)
            acc = add_there(acc, [pltpu.roll(v, 1, 1) for v in f])
            f = face(here, [pltpu.roll(v, ny - 1, 0) for v in here], wy)
            acc = add_here(acc, f)
            acc = add_there(acc, [pltpu.roll(v, 1, 0) for v in f])
            later = None
            if x + 1 < nx:
                here, old = plane(x + 1), here
                f = face(old, here)
                acc = add_here(acc, f)
                later = turn(f)
            for q in range(9):
                accs[q][x * ny : (x + 1) * ny, :] = acc[q]
            acc = later

    def sweeps(info, own, tiles_x, tiles_y, base, ext):
        odd_x, odd_y = info[4] > 0.5, info[5] > 0.5
        ext[...] = jnp.zeros_like(ext)

        def grab(ref, f, at):
            return ref[at + f * cells : at + (f + 1) * cells, :]

        def place(f, sx, sy, tile):
            xs = {-1: range(cx - W, cx), 0: range(cx), 1: range(W)}[sx]
            lo, hi, to = {-1: (cy - W, cy, 0), 0: (0, cy, W), 1: (0, W, W + cy)}[sy]
            at = {-1: 0, 0: W, 1: W + cx}[sx]
            for k, x in enumerate(xs):
                ext[f * ex + at + k, to : to + hi - lo, :] = tile[x * cy + lo : x * cy + hi, :]

        for f in range(3):
            place(f, 0, 0, own[f])
            for sy in (-1, 1):
                tile = pick(odd_y, (sy + 1) // 2, [grab(r, f, base[1]) for r in tiles_y])
                place(f, 0, sy, tile)
            for sx in (-1, 1):
                tile = pick(odd_x, (sx + 1) // 2, [grab(r, f, base[0]) for r in tiles_x])
                place(f, sx, 0, tile)
                for sy in (-1, 1):
                    along = [
                        pick(
                            odd_y,
                            (sy + 1) // 2,
                            [grab(r, f, base[0] + 3 * cells * (1 + b)) for b in range(uy)],
                        )
                        for r in tiles_x
                    ]
                    place(f, sx, sy, pick(odd_x, (sx + 1) // 2, along))
        lane = iota((ey, nz), 1)
        has_low, has_high = lane >= R, lane < nz - R
        src = [ext[x] for x in range(ex)]
        tem = [ext[ex + x] for x in range(ex)]
        con = [ext[2 * ex + x] for x in range(ex)]
        inv = [1.0 / (SINK + 6.0 * c) for c in con]
        for s in range(1, W + 1):
            new = list(tem)
            for x in range(s, ex - s):
                t = tem[x]
                total = tem[x - 1] + tem[x + 1]
                total = total + (pltpu.roll(t, 1, 0) + pltpu.roll(t, ey - 1, 0))
                total = total + jnp.where(has_low, pltpu.roll(t, R, 1), 0.0)
                total = total + jnp.where(has_high, pltpu.roll(t, nz - R, 1), 0.0)
                new[x] = (src[x] + con[x] * total) * inv[x]
            tem = new
        return [tem[W + x][W : W + cy, :] for x in range(cx)]

    def outer_kernel(k, split):
        first = k == 0

        def kernel(info, state, ins, ele, dop, cond, *rest):
            rest = list(rest)
            take = lambda c: [rest.pop(0) for _ in range(c)]
            accs = take(9)
            got0 = take(ux + uy)
            got = got0 if first else take(ux + uy)
            (tile,) = take(1)
            if not split:
                out, *faces = take(1 + ux)
                sends = take(uy)
            tile_out, rim_x, rim_y, temp, heat, ext, mobs = take(7)
            odd_x, odd_y = info[4] > 0.5, info[5] > 0.5

            if first:
                temp[...] = tile[...]
            else:
                own = [tile[f * cells : (f + 1) * cells, :] for f in range(3)]
                rows = sweeps(info, own, got[:ux], got[ux:], (3 * ny, 3 * nx), ext)
                for x in range(cx):
                    temp[x * cy : (x + 1) * cy, :] = rows[x]
            mobs[...] = 1.0 / (1.0 + DROP * temp[...])

            def side(axis, which, f):
                src = got0 if f == 3 else got
                if axis == 0:
                    return pick(odd_x, which, [r[f * ny : (f + 1) * ny, :] for r in src[:ux]])
                return pick(odd_y, which, [r[f * nx : (f + 1) * nx, :] for r in src[ux:]])

            def edge(rows):
                return [state[f, rows, :] for f in range(3)] + [epsof(ins[rows, :])]

            at = [
                (0, 0, slice(0, ny)), (0, 1, slice(nodes - ny, nodes)),
                (1, 0, pl.ds(0, nx, stride=ny)), (1, 1, pl.ds(ny - 1, nx, stride=ny)),
            ]
            for axis, which, rows in at:
                there = [side(axis, which, f) for f in range(4)]
                here = edge(rows)
                weight = info[2 * axis + which]
                f = face(here, there, weight) if which else turn(face(there, here, weight))
                for q, v in enumerate(f):
                    (rim_y if axis else rim_x)[9 * which + q] = v

            hsum = None
            for x in range(nx):
                rows = slice(x * ny, (x + 1) * ny)
                if split:
                    (h,) = whole(accs, rim_x, rim_y, x, [8])
                    h = h / (state[1, rows, :] + state[2, rows, :])
                else:
                    if x % R == 0:
                        mob = spread_rows(mobs, (x // R) * cy, cy)
                        dopx = spread_rows(dop, (x // R) * cy, cy)
                    here = [state[0, rows, :], state[1, rows, :], state[2, rows, :], None]
                    acc = whole(accs, rim_x, rim_y, x, range(9))
                    psi, n, p, h = solve(here, acc, ele[rows, :] == 1, dopx, mob)
                    out[0, rows, :] = psi
                    out[1, rows, :] = n
                    out[2, rows, :] = p
                hsum = h if x % R == 0 else hsum + h
                if x % R == R - 1:
                    xc = x // R
                    heat[xc * ny : (xc + 1) * ny, :] = hsum

            v = heat[pl.ds(0, cells, stride=R), :]
            for j in range(1, R):
                v = v + heat[pl.ds(j, cells, stride=R), :]
            lane = iota((cells, nz), 1)
            step = 1
            while step < R:
                v = v + jnp.where(
                    lane % (2 * step) < step, pltpu.roll(v, nz - step, 1), pltpu.roll(v, step, 1)
                )
                step *= 2
            tile_out[0:cells, :] = (GAIN * 0.5 / R**3) * mobs[...] * v
            tile_out[cells : 2 * cells, :] = temp[...]
            tile_out[2 * cells : 3 * cells, :] = cond[...]
            if not split:
                fields = [out.at[f] for f in range(3)]
                put_x(info, fields, faces)
                put_y(info, fields, sends)
                for s in sends:
                    s[3 * nx : 3 * nx + 3 * cells, :] = tile_out[...]

        return kernel

    def solve_kernel(info, state, ele, dop, tile, *rest):
        accs, (rim_x, rim_y, out, mobs) = rest[:9], rest[9:]
        mobs[...] = 1.0 / (1.0 + DROP * tile[cells : 2 * cells, :])
        for x in range(nx):
            rows = slice(x * ny, (x + 1) * ny)
            if x % R == 0:
                mob = spread_rows(mobs, (x // R) * cy, cy)
                dopx = spread_rows(dop, (x // R) * cy, cy)
            here = [state[0, rows, :], state[1, rows, :], state[2, rows, :], None]
            acc = whole(accs, rim_x, rim_y, x, range(8)) + [None]
            psi, n, p, _ = solve(here, acc, ele[rows, :] == 1, dopx, mob)
            out[0, rows, :] = psi
            out[1, rows, :] = n
            out[2, rows, :] = p

    def join_kernel(has_faces, base_y):
        def kernel(info, *rest):
            rest = list(rest)
            take = lambda c: [rest.pop(0) for _ in range(c)]
            faces = take(ux if has_faces else 0)
            (tile,) = take(1)
            got_y, sends = take(uy), take(ux)
            for k, s in enumerate(sends):
                at = 0
                if has_faces:
                    s[0 : 3 * ny, :] = faces[k][...]
                    at = 3 * ny
                s[at : at + 3 * cells, :] = tile[...]
                for b in range(uy):
                    at += 3 * cells
                    s[at : at + 3 * cells, :] = got_y[b][base_y : base_y + 3 * cells, :]

        return kernel

    def final_kernel(info, *rest):
        got, (tile, out, ext, flat) = rest[: ux + uy], rest[ux + uy :]
        own = [tile[f * cells : (f + 1) * cells, :] for f in range(3)]
        rows = sweeps(info, own, got[:ux], got[ux:], (0, 0), ext)
        for x in range(cx):
            flat[x * cy : (x + 1) * cy, :] = rows[x]
        coarse = nz // R
        sel = (iota((nz, coarse), 0) == R * iota((nz, coarse), 1)).astype(F32)
        out[...] = jnp.dot(
            flat[...], sel, precision=lax.Precision.HIGHEST, preferred_element_type=F32
        )

    def along(axis, pairings, sends):
        return [lax.ppermute(s, axis, pairs) for s, pairs in zip(sends, pairings)]

    def per_device(sol, ins, ele, zone, cat, warm):
        state = sol.reshape(3, nodes, nz)
        ins = ins.reshape(nodes, nz)
        ele = ele.reshape(nodes, nz)
        coarse = nz // R
        ix, iy = lax.axis_index("gx"), lax.axis_index("gy")
        info = jnp.stack(
            [ix > 0, ix < gx - 1, iy > 0, iy < gy - 1, ix % 2 == 1, iy % 2 == 1]
        ).astype(F32)
        work = nodes * nz
        V = pltpu.VMEM
        res = call(
            pack_kernel,
            [(4 * ny, nz)] * ux + [(4 * nx, nz)] * uy + [(cells, nz)] * 3,
            [V((3, nodes, nz), F32), V((nodes, nz), F32), V((nodes, nz), jnp.int32),
             pltpu.SemaphoreType.DMA((2,))],
            [info, state, ins, zone.reshape(cells, coarse), cat.reshape(cells, coarse),
             warm.reshape(cells, coarse)],
            work,
            specs=[smem, hbm, hbm, vmem, vmem, vmem],
        )
        sends, (dop, cond, tile) = res[: ux + uy], res[ux + uy :]
        got0 = along("gx", px, sends[:ux]) + along("gy", py, sends[ux:])
        got_y, faces = [], []
        for k in range(NEWTON):
            last = k == NEWTON - 1
            accs = call(inner_kernel, [(nodes, nz)] * 9, [], [info, state, ins], 200 * work)
            got = []
            if k:
                joined = call(
                    join_kernel(True, 3 * nx),
                    [(3 * ny + 3 * cells * (1 + uy), nz)] * ux,
                    [],
                    [info] + faces + [tile] + got_y,
                    work,
                )
                got = along("gx", px, joined) + got_y
            args = [info, state, ins, ele, dop, cond] + accs + got0 + got + [tile]
            outs = []
            if not last:
                outs += [(3, nodes, nz)] + [(3 * ny, nz)] * ux + [(3 * nx + 3 * cells, nz)] * uy
            outs += [(3 * cells, nz)]
            rims = [(18, ny, nz), (18, nx, nz)]
            scratch = [
                V((cells, nz), F32), V((cx * ny, nz), F32), V((3 * ex, ey, nz), F32),
                V((cells, nz), F32),
            ]
            if last:
                outs += rims
            else:
                scratch = [V(r, F32) for r in rims] + scratch
            res = call(outer_kernel(k, last), outs, scratch, args, 100 * work)
            if last:
                tile = res[0]
                got_y = along("gy", py, [tile] * uy)
                (state,) = call(
                    solve_kernel, [(3, nodes, nz)], [V((cells, nz), F32)],
                    [info, state, ele, dop, tile] + accs + res[1:], 100 * work,
                )
            else:
                state, faces, sends, tile = res[0], res[1 : 1 + ux], res[1 + ux : -1], res[-1]
                got_y = along("gy", py, sends)
        joined = call(
            join_kernel(False, 0), [(3 * cells * (1 + uy), nz)] * ux, [],
            [info, tile] + got_y, work,
        )
        got = along("gx", px, joined) + got_y
        (warm,) = call(
            final_kernel,
            [(cells, coarse)],
            [V((3 * ex, ey, nz), F32), V((cells, nz), F32)],
            [info] + got + [tile],
            work,
        )
        return state.reshape(3, nx, ny, nz), warm.reshape(cx, cy, coarse)

    return per_device


def solution(mesh):
    placed = (
        P(None, "gx", "gy", None),
        P("gx", "gy", None),
        P("gx", "gy", None),
        P("gx", "gy", None),
        P("gx", "gy", None),
        P("gx", "gy", None),
    )
    gx, gy = mesh.shape["gx"], mesh.shape["gy"]

    def body(sol, *rest):
        _, nx, ny, nz = sol.shape
        return make(nx, ny, nz, gx, gy)(sol, *rest)

    return jax.shard_map(
        body,
        mesh=mesh,
        in_specs=placed,
        out_specs=(P(None, "gx", "gy", None), P("gx", "gy", None)),
        check_vma=False,
    )
```

```python
import jax
import jax.numpy as jnp
from jax import lax
from jax.experimental import pallas as pl
from jax.experimental.pallas import tpu as pltpu
from jax.sharding import PartitionSpec as P

R = 4
NEWTON = 3
SWEEPS = 3

POISSON = 2.0
CHARGE = 4.0
SHIFT = 24.0
BIAS = 0.25
GAIN = 1.0
SINK = 0.3
DROP = 0.5
DOPING = (-2.0, -0.5, 0.5, 2.0)
CONDUCT = (0.5, 1.0, 2.0, 4.0)

F32 = jnp.float32


def phases(count):
    out = []
    for start in (0, 1):
        pairs = []
        for i in range(start, count - 1, 2):
            pairs += [(i, i + 1), (i + 1, i)]
        if pairs:
            out.append(pairs)
    return out


def both(pairs_x, pairs_y, count_y):
    return [(i * count_y + j, k * count_y + m) for i, k in pairs_x for j, m in pairs_y]


def lookup(labels, table):
    value = jnp.full(labels.shape, table[0], F32)
    for level in range(1, len(table)):
        value = jnp.where(labels == level, table[level], value)
    return value


def face(here, there, weight=None):
    psi_i, n_i, p_i, e_i = here
    psi_j, n_j, p_j, e_j = there
    d = psi_j - psi_i
    small = jnp.abs(d) < 0.25
    r = 1.0 / jnp.where(small, 1.0, jnp.exp(d) - 1.0)
    q = d * d
    b = jnp.where(
        small, (1.0 - 0.5 * d) + q * (1 / 12 - q * (1 / 720 - q * (1 / 30240))), d * r
    )
    bm = b + d
    s = jnp.where(small, -0.5 + d * (1 / 6 - q * (1 / 180 - q * (1 / 5040))), r * (1.0 - bm))
    e = 0.5 * (e_i + e_j)
    if weight is None:
        gn = n_i + (n_i - n_j) * s
        gp = (p_i - p_j) * s - p_j
    else:
        b = b * weight
        bm = b + d * weight
        s = s * weight
        e = e * weight
        gn = n_i * weight + (n_i - n_j) * s
        gp = (p_i - p_j) * s - p_j * weight
    fe = n_j * b - n_i * bm
    fh = p_j * bm - p_i * b
    j = fe - fh
    return e * d, e, fe, fh, gn, gp, b, bm, j * j


def add_here(acc, f):
    lap, es, fe, fh, gn, gp, b, bm, h = f
    return [x + y for x, y in zip(acc, (lap, es, fe, fh, gn, gp, b, bm, h))]


def add_there(acc, f):
    lap, es, fe, fh, gn, gp, b, bm, h = f
    return [
        acc[0] - lap, acc[1] + es, acc[2] - fe, acc[3] - fh,
        acc[4] + gn, acc[5] + gp, acc[6] + bm, acc[7] + b, acc[8] + h,
    ]


def solve(here, acc, contact, dop, mob):
    psi, n, p, _ = here
    lap, es, fe, fh, gn, gp, fwd, bwd, h = acc
    total = n + p
    rden = 1.0 / (total + 2.0)
    rec = (n * p - 1.0) * rden
    rn = (p + 1.0) * rden
    rn = rn * rn
    rp = (n + 1.0) * rden
    rp = rp * rp
    r0 = POISSON * lap + CHARGE * (p - n + dop)
    r1 = mob * fe - rec
    r2 = mob * fh - rec
    a = -POISSON * es
    b1 = mob * gn
    b2 = -mob * bwd - rn - SHIFT
    g1 = mob * gp
    g3 = -mob * fwd - rp - SHIFT
    caa = b2 * g3 - rp * rn
    cab = -(rp * g1 + b1 * g3)
    cac = -(b1 * rn + b2 * g1)
    rdet = 1.0 / (a * caa + CHARGE * (cac - cab))
    cb1 = CHARGE * b1
    cg1 = CHARGE * g1
    s0 = (caa * r0 + CHARGE * ((g3 - rn) * r1 + (rp - b2) * r2)) * rdet
    s1 = (cab * r0 + (a * g3 - cg1) * r1 + (cb1 + a * rp) * r2) * rdet
    s2 = (cac * r0 + (a * rn - cg1) * r1 + (a * b2 + cb1) * r2) * rdet
    s0 = jnp.where(contact, psi - BIAS * dop, s0)
    s1 = jnp.where(contact, n - 1.0, s1)
    s2 = jnp.where(contact, p - 1.0, s2)
    heat = None if h is None else h / total
    return psi - s0, n * jnp.exp(-s1 / n), p * jnp.exp(-s2 / p), heat


def iota(shape, axis):
    return lax.broadcasted_iota(jnp.int32, shape, axis)


def spread_rows(ref, first, count):
    lanes = ref.shape[-1]
    group = iota((count * R, lanes), 0) // R
    out = jnp.broadcast_to(ref[first : first + 1, :], (count * R, lanes))
    for j in range(1, count):
        out = jnp.where(group == j, ref[first + j : first + j + 1, :], out)
    return out


def make(nx, ny, nz, gx, gy):
    cx, cy = nx // R, ny // R
    cells = cx * cy
    W = SWEEPS
    px, py = phases(gx), phases(gy)
    ux, uy = len(px), len(py)
    ex, ey = cx + 2 * W, -(-(cy + 2 * W) // 8) * 8
    nodes = nx * ny
    params = pltpu.CompilerParams(vmem_limit_bytes=16 * 1024 * 1024)
    vmem = pl.BlockSpec(memory_space=pltpu.VMEM)
    deep = {True: (W - 1, W, W - 1), False: (W - 1, W)}
    wide = {f: sum(deep[f]) for f in deep}

    def call(kernel, outs, scratch, args, cost):
        return list(
            pl.pallas_call(
                kernel,
                out_shape=[jax.ShapeDtypeStruct(s, F32) for s in outs],
                in_specs=[vmem] * len(args),
                out_specs=[vmem] * len(outs),
                scratch_shapes=scratch,
                compiler_params=params,
                cost_estimate=pl.CostEstimate(flops=cost, bytes_accessed=0, transcendentals=0),
            )(*args)
        )

    def place_of():
        ix, iy = lax.axis_index("gx"), lax.axis_index("gy")
        some = lambda test: jnp.where(test, 1.0, 0.0)
        weights = [some(ix > 0), some(ix < gx - 1), some(iy > 0), some(iy < gy - 1)]
        return ix % 2 == 1, iy % 2 == 1, weights

    def pick(odd, which, values):
        get = lambda k: values[k] if k < len(values) else jnp.zeros_like(values[0])
        return jnp.where(odd, get(which), get(1 - which))

    def put_x(odd, fields, sends):
        for f, ref in enumerate(fields):
            low, high = ref[0:ny, :], ref[(nx - 1) * ny : nodes, :]
            for k, send in enumerate(sends):
                first, second = (low, high) if k == 0 else (high, low)
                send[f * ny : (f + 1) * ny, :] = jnp.where(odd, first, second)

    def put_y(odd, fields, sends):
        for f, ref in enumerate(fields):
            low = ref[pl.ds(0, nx, stride=ny), :]
            high = ref[pl.ds(ny - 1, nx, stride=ny), :]
            for k, send in enumerate(sends):
                first, second = (low, high) if k == 0 else (high, low)
                send[f * nx : (f + 1) * nx, :] = jnp.where(odd, first, second)

    def put_cells_y(odd, fresh, fields, sends, at):
        for (ref, base), depth in zip(fields, deep[fresh]):
            for i in range(depth):
                low = ref[pl.ds(base + i, cx, stride=cy), :]
                high = ref[pl.ds(base + cy - depth + i, cx, stride=cy), :]
                for k, send in enumerate(sends):
                    first, second = (low, high) if k == 0 else (high, low)
                    send[at : at + cx, :] = jnp.where(odd, first, second)
                at += cx

    def put_cells_x(odd, fresh, fields, sends, at):
        for (ref, base), depth in zip(fields, deep[fresh]):
            low = ref[base : base + depth * cy, :]
            high = ref[base + cells - depth * cy : base + cells, :]
            for k, send in enumerate(sends):
                first, second = (low, high) if k == 0 else (high, low)
                send[at : at + depth * cy, :] = jnp.where(odd, first, second)
            at += depth * cy
        return at

    def turn(f):
        lap, es, fe, fh, gn, gp, b, bm, h = f
        return [-lap, es, -fe, -fh, gn, gp, bm, b, h]

    def whole(accs, rim_x, rim_y, x, qs):
        row = iota((8, nz), 0)
        out = []
        for q in qs:
            a = accs[q][x * ny : (x + 1) * ny, :]
            if x == 0:
                a = a + rim_x[q]
            if x == nx - 1:
                a = a + rim_x[9 + q]
            parts = [a[r : r + 8] for r in range(0, ny, 8)]
            parts[0] = parts[0] + jnp.where(row == 0, rim_y[q, x : x + 1, :], 0.0)
            parts[-1] = parts[-1] + jnp.where(row == 7, rim_y[9 + q, x : x + 1, :], 0.0)
            out.append(jnp.concatenate(parts, 0) if len(parts) > 1 else parts[0])
        return out

    def pack_kernel(start, *sends):
        odd_x, odd_y, _ = place_of()
        fields = [start.at[f] for f in range(4)]
        put_x(odd_x, fields, sends[:ux])
        put_y(odd_y, fields, sends[ux:])

    def table_kernel(after, zone, cat, warm, dop, cond, temp):
        coarse = nz // R
        pickz = (iota((coarse, nz), 1) // R == iota((coarse, nz), 0)).astype(F32)

        def widen(x):
            return jnp.dot(x, pickz, precision=lax.Precision.HIGHEST, preferred_element_type=F32)

        dop[...] = widen(lookup(zone[...], DOPING))
        cond[...] = widen(lookup(cat[...], CONDUCT))
        temp[...] = widen(warm[...])

    def inner_kernel(state, eps, *accs):
        zlane = iota((ny, nz), 1)
        wz = jnp.where(zlane < nz - 1, 1.0, 0.0)
        wy = jnp.where(iota((ny, nz), 0) < ny - 1, 1.0, 0.0)

        def plane(x):
            rows = slice(x * ny, (x + 1) * ny)
            return [state[0, rows, :], state[1, rows, :], state[2, rows, :], eps[3, rows, :]]

        here = plane(0)
        acc = None
        for x in range(nx):
            f = face(here, [pltpu.roll(v, nz - 1, 1) for v in here], wz)
            acc = list(f) if acc is None else add_here(acc, f)
            acc = add_there(acc, [pltpu.roll(v, 1, 1) for v in f])
            f = face(here, [pltpu.roll(v, ny - 1, 0) for v in here], wy)
            acc = add_here(acc, f)
            acc = add_there(acc, [pltpu.roll(v, 1, 0) for v in f])
            later = None
            if x + 1 < nx:
                here, old = plane(x + 1), here
                f = face(old, here)
                acc = add_here(acc, f)
                later = turn(f)
            for q in range(9):
                accs[q][x * ny : (x + 1) * ny, :] = acc[q]
            acc = later

    def sweeps(fresh, own, tiles_x, tiles_y, base, ext, cext):
        odd_x, odd_y, _ = place_of()
        grids = [(ext, 0), (ext, ex), (cext, 0)]
        ext[...] = jnp.zeros_like(ext)
        if fresh:
            cext[...] = jnp.zeros_like(cext)
        past = base[0] + wide[fresh] * cy
        off_x, off_y = base[0], base[1]
        gone = 0
        for f, depth in enumerate(deep[fresh]):
            (ref, row), (grid, g) = own[f], grids[f]
            for x in range(cx):
                grid[g + W + x, W : W + cy, :] = ref[row + x * cy : row + (x + 1) * cy, :]
            for sy in (0, 1):
                to = W + cy if sy else W - depth
                for x in range(cx):
                    tile = pick(
                        odd_y, sy, [r[pl.ds(off_y + x, depth, stride=cx), :] for r in tiles_y]
                    )
                    grid[g + W + x, to : to + depth, :] = tile
            for sx in (0, 1):
                to = W + cx if sx else W - depth
                tile = pick(odd_x, sx, [r[off_x : off_x + depth * cy, :] for r in tiles_x])
                for i in range(depth):
                    grid[g + to + i, W : W + cy, :] = tile[i * cy : (i + 1) * cy]
                near = depth - 1
                for i in range(near):
                    x = i if sx else cx - near + i
                    at = W + cx + i if sx else W - near + i
                    for sy in (0, 1):
                        skip = 0 if sy else depth - near
                        along = [
                            pick(
                                odd_y,
                                sy,
                                [
                                    r[
                                        pl.ds(
                                            past + b * wide[fresh] * cx + gone + skip * cx + x,
                                            near,
                                            stride=cx,
                                        ),
                                        :,
                                    ]
                                    for b in range(uy)
                                ],
                            )
                            for r in tiles_x
                        ]
                        to_y = W + cy if sy else W - near
                        grid[g + at, to_y : to_y + near, :] = pick(odd_x, sx, along)
            off_x += depth * cy
            off_y += depth * cx
            gone += depth * cx
        lane = iota((ey, nz), 1)
        has_low, has_high = lane >= R, lane < nz - R
        src = [ext[x] for x in range(ex)]
        tem = [ext[ex + x] for x in range(ex)]
        con = [cext[x] for x in range(ex)]
        inv = [1.0 / (SINK + 6.0 * c) for c in con]
        for s in range(1, W + 1):
            new = list(tem)
            for x in range(s, ex - s):
                t = tem[x]
                total = tem[x - 1] + tem[x + 1]
                total = total + (pltpu.roll(t, 1, 0) + pltpu.roll(t, ey - 1, 0))
                total = total + jnp.where(has_low, pltpu.roll(t, R, 1), 0.0)
                total = total + jnp.where(has_high, pltpu.roll(t, nz - R, 1), 0.0)
                new[x] = (src[x] + con[x] * total) * inv[x]
            tem = new
        return [tem[W + x][W : W + cy, :] for x in range(cx)]

    def outer_kernel(k, split):
        first, fresh = k == 0, k == 1

        def kernel(state, eps, ele, dop, cond, *rest):
            rest = list(rest)
            take = lambda c: [rest.pop(0) for _ in range(c)]
            accs = take(9)
            got0 = take(ux + uy)
            got = got0 if first else take(ux + uy)
            (tile,) = take(1)
            cext = None if first or fresh else take(1)[0]
            if not split:
                out, *faces = take(1 + ux)
            sends = take(uy)
            (tile_out,) = take(1)
            if fresh:
                (cext,) = take(1)
            rim_x, rim_y, temp, heat, ext, mobs = take(6)
            odd_x, odd_y, weights = place_of()

            if first:
                temp[...] = tile[...]
            else:
                own = [(tile, 0), (tile, cells), (cond, 0)]
                rows = sweeps(fresh, own, got[:ux], got[ux:], (3 * ny, 3 * nx), ext, cext)
                for x in range(cx):
                    temp[x * cy : (x + 1) * cy, :] = rows[x]
            mobs[...] = 1.0 / (1.0 + DROP * temp[...])

            def side(axis, which, f):
                src = got0 if f == 3 else got
                if axis == 0:
                    return pick(odd_x, which, [r[f * ny : (f + 1) * ny, :] for r in src[:ux]])
                return pick(odd_y, which, [r[f * nx : (f + 1) * nx, :] for r in src[ux:]])

            def edge(rows):
                return [state[f, rows, :] for f in range(3)] + [eps[3, rows, :]]

            at = [
                (0, 0, slice(0, ny)), (0, 1, slice(nodes - ny, nodes)),
                (1, 0, pl.ds(0, nx, stride=ny)), (1, 1, pl.ds(ny - 1, nx, stride=ny)),
            ]
            for axis, which, rows in at:
                there = [side(axis, which, f) for f in range(4)]
                here = edge(rows)
                weight = weights[2 * axis + which]
                f = face(here, there, weight) if which else turn(face(there, here, weight))
                for q, v in enumerate(f):
                    (rim_y if axis else rim_x)[9 * which + q] = v

            hsum = None
            for x in range(nx):
                rows = slice(x * ny, (x + 1) * ny)
                if split:
                    (h,) = whole(accs, rim_x, rim_y, x, [8])
                    h = h / (state[1, rows, :] + state[2, rows, :])
                else:
                    if x % R == 0:
                        mob = spread_rows(mobs, (x // R) * cy, cy)
                        dopx = spread_rows(dop, (x // R) * cy, cy)
                    here = [state[0, rows, :], state[1, rows, :], state[2, rows, :], None]
                    acc = whole(accs, rim_x, rim_y, x, range(9))
                    psi, n, p, h = solve(here, acc, ele[rows, :] == 1, dopx, mob)
                    out[0, rows, :] = psi
                    out[1, rows, :] = n
                    out[2, rows, :] = p
                hsum = h if x % R == 0 else hsum + h
                if x % R == R - 1:
                    xc = x // R
                    heat[xc * ny : (xc + 1) * ny, :] = hsum

            v = heat[pl.ds(0, cells, stride=R), :]
            for j in range(1, R):
                v = v + heat[pl.ds(j, cells, stride=R), :]
            lane = iota((cells, nz), 1)
            step = 1
            while step < R:
                v = v + jnp.where(
                    lane % (2 * step) < step, pltpu.roll(v, nz - step, 1), pltpu.roll(v, step, 1)
                )
                step *= 2
            tile_out[0:cells, :] = (GAIN * 0.5 / R**3) * mobs[...] * v
            tile_out[cells : 2 * cells, :] = temp[...]
            at = 0
            if not split:
                fields = [out.at[f] for f in range(3)]
                put_x(odd_x, fields, faces)
                put_y(odd_y, fields, sends)
                at = 3 * nx
            parts = [(tile_out, 0), (tile_out, cells), (cond, 0)]
            put_cells_y(odd_y, first, parts, sends, at)

        return kernel

    def solve_kernel(state, ele, dop, tile, *rest):
        accs, (rim_x, rim_y, out, token, mobs) = rest[:9], rest[9:]
        token[...] = jnp.zeros_like(token)
        mobs[...] = 1.0 / (1.0 + DROP * tile[cells : 2 * cells, :])
        for x in range(nx):
            rows = slice(x * ny, (x + 1) * ny)
            if x % R == 0:
                mob = spread_rows(mobs, (x // R) * cy, cy)
                dopx = spread_rows(dop, (x // R) * cy, cy)
            here = [state[0, rows, :], state[1, rows, :], state[2, rows, :], None]
            acc = whole(accs, rim_x, rim_y, x, range(8)) + [None]
            psi, n, p, _ = solve(here, acc, ele[rows, :] == 1, dopx, mob)
            out[0, rows, :] = psi
            out[1, rows, :] = n
            out[2, rows, :] = p

    def join_kernel(fresh, has_faces):
        def kernel(after, cond, tile, *rest):
            rest = list(rest)
            take = lambda c: [rest.pop(0) for _ in range(c)]
            faces = take(ux if has_faces else 0)
            got_y, sends = take(uy), take(ux)
            odd_x, _, _ = place_of()
            at = base = 0
            if has_faces:
                at, base = 3 * ny, 3 * nx
                for k, s in enumerate(sends):
                    s[0:at, :] = faces[k][...]
            parts = [(tile, 0), (tile, cells), (cond, 0)]
            at = put_cells_x(odd_x, fresh, parts, sends, at)
            more = wide[fresh] * cx
            for k, s in enumerate(sends):
                for b in range(uy):
                    s[at + b * more : at + (b + 1) * more, :] = got_y[b][base : base + more, :]

        return kernel

    def final_kernel(cext, *rest):
        got, (tile, out, ext, flat) = rest[: ux + uy], rest[ux + uy :]
        own = [(tile, 0), (tile, cells)]
        rows = sweeps(False, own, got[:ux], got[ux:], (0, 0), ext, cext)
        for x in range(cx):
            flat[x * cy : (x + 1) * cy, :] = rows[x]
        coarse = nz // R
        sel = (iota((nz, coarse), 0) == R * iota((nz, coarse), 1)).astype(F32)
        out[...] = jnp.dot(
            flat[...], sel, precision=lax.Precision.HIGHEST, preferred_element_type=F32
        )

    def along(axis, pairings, sends):
        return [lax.ppermute(s, axis, pairs) for s, pairs in zip(sends, pairings)]

    def per_device(sol, ins, ele, zone, cat, warm):
        ele = ele.reshape(nodes, nz)
        coarse = nz // R
        work = nodes * nz
        V = pltpu.VMEM
        eps = jnp.where(ins.reshape(1, nodes, nz) == 1, 0.4, 1.0).astype(F32)
        state = eps = jnp.concatenate([sol.reshape(3, nodes, nz), eps], 0)
        sends = call(
            pack_kernel, [(4 * ny, nz)] * ux + [(4 * nx, nz)] * uy, [], [state], work
        )
        dop, cond, tile = call(
            table_kernel, [(cells, nz)] * 3, [],
            [sends[0], zone.reshape(cells, coarse), cat.reshape(cells, coarse),
             warm.reshape(cells, coarse)],
            work,
        )
        got0 = along("gx", px, sends[:ux]) + along("gy", py, sends[ux:])
        got_y, faces, cext = [], [], []
        for k in range(NEWTON):
            first, fresh, last = k == 0, k == 1, k == NEWTON - 1
            accs = call(inner_kernel, [(nodes, nz)] * 9, [], [state, eps], 200 * work)
            got = []
            if not first:
                joined = call(
                    join_kernel(fresh, True),
                    [(3 * ny + wide[fresh] * (cy + cx * uy), nz)] * ux,
                    [],
                    [accs[0], cond, tile] + faces + got_y,
                    work,
                )
                got = along("gx", px, joined) + got_y
            args = [state, eps, ele, dop, cond] + accs + got0 + got + [tile]
            outs = []
            if not (first or fresh):
                args += cext
            if not last:
                outs += [(3, nodes, nz)] + [(3 * ny, nz)] * ux
            outs += [((0 if last else 3 * nx) + wide[first] * cx, nz)] * uy
            outs += [(2 * cells, nz)]
            if fresh:
                outs += [(ex, ey, nz)]
            rims = [(18, ny, nz), (18, nx, nz)]
            scratch = [
                V((cells, nz), F32), V((cx * ny, nz), F32), V((2 * ex, ey, nz), F32),
                V((cells, nz), F32),
            ]
            if last:
                outs += rims
            else:
                scratch = [V(r, F32) for r in rims] + scratch
            res = call(outer_kernel(k, last), outs, scratch, args, 100 * work)
            take = lambda c: [res.pop(0) for _ in range(c)]
            if not last:
                state, *faces = take(1 + ux)
            got_y = along("gy", py, take(uy))
            (tile,) = take(1)
            if fresh:
                cext = take(1)
            if last:
                state, token = call(
                    solve_kernel, [(3, nodes, nz), (8, nz)], [V((cells, nz), F32)],
                    [state, ele, dop, tile] + accs + res, 100 * work,
                )
        joined = call(
            join_kernel(False, False), [(wide[False] * (cy + cx * uy), nz)] * ux, [],
            [token, cond, tile] + got_y, work,
        )
        got = along("gx", px, joined) + got_y
        (warm,) = call(
            final_kernel,
            [(cells, coarse)],
            [V((2 * ex, ey, nz), F32), V((cells, nz), F32)],
            cext + got + [tile],
            work,
        )
        return state.reshape(3, nx, ny, nz), warm.reshape(cx, cy, coarse)

    return per_device


def solution(mesh):
    placed = (
        P(None, "gx", "gy", None),
        P("gx", "gy", None),
        P("gx", "gy", None),
        P("gx", "gy", None),
        P("gx", "gy", None),
        P("gx", "gy", None),
    )
    gx, gy = mesh.shape["gx"], mesh.shape["gy"]

    def body(sol, *rest):
        _, nx, ny, nz = sol.shape
        return make(nx, ny, nz, gx, gy)(sol, *rest)

    return jax.shard_map(
        body,
        mesh=mesh,
        in_specs=placed,
        out_specs=(P(None, "gx", "gy", None), P("gx", "gy", None)),
        check_vma=False,
    )
```

```python
import jax
import jax.numpy as jnp
from jax import lax
from jax.experimental import pallas as pl
from jax.experimental.pallas import tpu as pltpu
from jax.sharding import PartitionSpec as P


R = 4
NEWTON = 3
SWEEPS = 3

POISSON = 2.0
CHARGE = 4.0
SHIFT = 24.0
BIAS = 0.25
GAIN = 1.0
SINK = 0.3
DROP = 0.5
DOPING = (-2.0, -0.5, 0.5, 2.0)
CONDUCT = (0.5, 1.0, 2.0, 4.0)

F32 = jnp.float32


def phases(count):
    out = []
    for start in (0, 1):
        pairs = []
        for i in range(start, count - 1, 2):
            pairs += [(i, i + 1), (i + 1, i)]
        if pairs:
            out.append(pairs)
    return out


def lookup(labels, table):
    value = jnp.full(labels.shape, table[0], F32)
    for level in range(1, len(table)):
        value = jnp.where(labels == level, table[level], value)
    return value


def face(here, there, weight=None):
    psi_i, n_i, p_i, e_i = here
    psi_j, n_j, p_j, e_j = there
    d = psi_j - psi_i
    small = jnp.abs(d) < 0.25
    r = 1.0 / jnp.where(small, 1.0, jnp.exp(d) - 1.0)
    q = d * d
    b = jnp.where(
        small, (1.0 - 0.5 * d) + q * (1 / 12 - q * (1 / 720 - q * (1 / 30240))), d * r
    )
    bm = b + d
    s = jnp.where(small, -0.5 + d * (1 / 6 - q * (1 / 180 - q * (1 / 5040))), r * (1.0 - bm))
    e = 0.5 * (e_i + e_j)
    if weight is None:
        gn = n_i + (n_i - n_j) * s
        gp = (p_i - p_j) * s - p_j
    else:
        b = b * weight
        bm = b + d * weight
        s = s * weight
        e = e * weight
        gn = n_i * weight + (n_i - n_j) * s
        gp = (p_i - p_j) * s - p_j * weight
    fe = n_j * b - n_i * bm
    fh = p_j * bm - p_i * b
    j = fe - fh
    return e * d, e, fe, fh, gn, gp, b, bm, j * j


def add_here(acc, f):
    lap, es, fe, fh, gn, gp, b, bm, h = f
    return [x + y for x, y in zip(acc, (lap, es, fe, fh, gn, gp, b, bm, h))]


def add_there(acc, f):
    lap, es, fe, fh, gn, gp, b, bm, h = f
    return [
        acc[0] - lap, acc[1] + es, acc[2] - fe, acc[3] - fh,
        acc[4] + gn, acc[5] + gp, acc[6] + bm, acc[7] + b, acc[8] + h,
    ]


def solve(here, acc, contact, dop, mob):
    psi, n, p, _ = here
    lap, es, fe, fh, gn, gp, fwd, bwd, h = acc
    total = n + p
    rden = 1.0 / (total + 2.0)
    rec = (n * p - 1.0) * rden
    rn = (p + 1.0) * rden
    rn = rn * rn
    rp = (n + 1.0) * rden
    rp = rp * rp
    r0 = POISSON * lap + CHARGE * (p - n + dop)
    r1 = mob * fe - rec
    r2 = mob * fh - rec
    a = -POISSON * es
    b1 = mob * gn
    b2 = -mob * bwd - rn - SHIFT
    g1 = mob * gp
    g3 = -mob * fwd - rp - SHIFT
    caa = b2 * g3 - rp * rn
    cab = -(rp * g1 + b1 * g3)
    cac = -(b1 * rn + b2 * g1)
    rdet = 1.0 / (a * caa + CHARGE * (cac - cab))
    cb1 = CHARGE * b1
    cg1 = CHARGE * g1
    s0 = (caa * r0 + CHARGE * ((g3 - rn) * r1 + (rp - b2) * r2)) * rdet
    s1 = (cab * r0 + (a * g3 - cg1) * r1 + (cb1 + a * rp) * r2) * rdet
    s2 = (cac * r0 + (a * rn - cg1) * r1 + (a * b2 + cb1) * r2) * rdet
    s0 = jnp.where(contact, psi - BIAS * dop, s0)
    s1 = jnp.where(contact, n - 1.0, s1)
    s2 = jnp.where(contact, p - 1.0, s2)
    heat = None if h is None else h / total
    return psi - s0, n * jnp.exp(-s1 / n), p * jnp.exp(-s2 / p), heat


def iota(shape, axis):
    return lax.broadcasted_iota(jnp.int32, shape, axis)


def spread_rows(ref, first, count):
    lanes = ref.shape[-1]
    group = iota((count * R, lanes), 0) // R
    out = jnp.broadcast_to(ref[first : first + 1, :], (count * R, lanes))
    for j in range(1, count):
        out = jnp.where(group == j, ref[first + j : first + j + 1, :], out)
    return out


def make(nx, ny, nz, gx, gy):
    cx, cy = nx // R, ny // R
    cells = cx * cy
    W = SWEEPS
    px, py = phases(gx), phases(gy)
    ux, uy = len(px), len(py)
    ex, ey = cx + 2 * W, -(-(cy + 2 * W) // 8) * 8
    nodes = nx * ny
    params = pltpu.CompilerParams(vmem_limit_bytes=16 * 1024 * 1024)
    vmem = pl.BlockSpec(memory_space=pltpu.VMEM)
    deep = {True: (W - 1, W, W - 1), False: (W - 1, W)}
    wide = {f: sum(deep[f]) for f in deep}

    def call(kernel, outs, scratch, args, cost):
        return list(
            pl.pallas_call(
                kernel,
                out_shape=[jax.ShapeDtypeStruct(s, F32) for s in outs],
                in_specs=[vmem] * len(args),
                out_specs=[vmem] * len(outs),
                scratch_shapes=scratch,
                compiler_params=params,
                cost_estimate=pl.CostEstimate(flops=cost, bytes_accessed=0, transcendentals=0),
            )(*args)
        )

    def place_of():
        ix, iy = lax.axis_index("gx"), lax.axis_index("gy")
        some = lambda test: jnp.where(test, 1.0, 0.0)
        weights = [some(ix > 0), some(ix < gx - 1), some(iy > 0), some(iy < gy - 1)]
        return ix % 2 == 1, iy % 2 == 1, weights

    def pick(odd, which, values):
        get = lambda k: values[k] if k < len(values) else jnp.zeros_like(values[0])
        return jnp.where(odd, get(which), get(1 - which))

    def put_x(odd, fields, sends):
        for f, ref in enumerate(fields):
            low, high = ref[0:ny, :], ref[(nx - 1) * ny : nodes, :]
            for k, send in enumerate(sends):
                first, second = (low, high) if k == 0 else (high, low)
                send[f * ny : (f + 1) * ny, :] = jnp.where(odd, first, second)

    def put_y(odd, fields, sends):
        for f, ref in enumerate(fields):
            low = ref[pl.ds(0, nx, stride=ny), :]
            high = ref[pl.ds(ny - 1, nx, stride=ny), :]
            for k, send in enumerate(sends):
                first, second = (low, high) if k == 0 else (high, low)
                send[f * nx : (f + 1) * nx, :] = jnp.where(odd, first, second)

    def put_cells_y(odd, fresh, fields, sends, at):
        for (ref, base), depth in zip(fields, deep[fresh]):
            for i in range(depth):
                low = ref[pl.ds(base + i, cx, stride=cy), :]
                high = ref[pl.ds(base + cy - depth + i, cx, stride=cy), :]
                for k, send in enumerate(sends):
                    first, second = (low, high) if k == 0 else (high, low)
                    send[at : at + cx, :] = jnp.where(odd, first, second)
                at += cx

    def put_cells_x(odd, fresh, fields, sends, at):
        for (ref, base), depth in zip(fields, deep[fresh]):
            low = ref[base : base + depth * cy, :]
            high = ref[base + cells - depth * cy : base + cells, :]
            for k, send in enumerate(sends):
                first, second = (low, high) if k == 0 else (high, low)
                send[at : at + depth * cy, :] = jnp.where(odd, first, second)
            at += depth * cy
        return at

    def turn(f):
        lap, es, fe, fh, gn, gp, b, bm, h = f
        return [-lap, es, -fe, -fh, gn, gp, bm, b, h]

    def whole(accs, rim_x, rim_y, x, qs):
        row = iota((8, nz), 0)
        out = []
        for q in qs:
            a = accs[q][x * ny : (x + 1) * ny, :]
            if x == 0:
                a = a + rim_x[q]
            if x == nx - 1:
                a = a + rim_x[9 + q]
            parts = [a[r : r + 8] for r in range(0, ny, 8)]
            parts[0] = parts[0] + jnp.where(row == 0, rim_y[q, x : x + 1, :], 0.0)
            parts[-1] = parts[-1] + jnp.where(row == 7, rim_y[9 + q, x : x + 1, :], 0.0)
            out.append(jnp.concatenate(parts, 0) if len(parts) > 1 else parts[0])
        return out

    def pack_kernel(start, *sends):
        odd_x, odd_y, _ = place_of()
        fields = [start.at[f] for f in range(4)]
        put_x(odd_x, fields, sends[:ux])
        put_y(odd_y, fields, sends[ux:])

    def table_kernel(after, zone, cat, warm, dop, cond, temp):
        coarse = nz // R
        pickz = (iota((coarse, nz), 1) // R == iota((coarse, nz), 0)).astype(F32)

        def widen(x):
            return jnp.dot(x, pickz, precision=lax.Precision.HIGHEST, preferred_element_type=F32)

        dop[...] = widen(lookup(zone[...], DOPING))
        cond[...] = widen(lookup(cat[...], CONDUCT))
        temp[...] = widen(warm[...])

    def inner_kernel(state, eps, *accs):
        zlane = iota((ny, nz), 1)
        wz = jnp.where(zlane < nz - 1, 1.0, 0.0)
        wy = jnp.where(iota((ny, nz), 0) < ny - 1, 1.0, 0.0)

        def plane(x):
            rows = slice(x * ny, (x + 1) * ny)
            return [state[0, rows, :], state[1, rows, :], state[2, rows, :], eps[3, rows, :]]

        here = plane(0)
        acc = None
        for x in range(nx):
            f = face(here, [pltpu.roll(v, nz - 1, 1) for v in here], wz)
            acc = list(f) if acc is None else add_here(acc, f)
            acc = add_there(acc, [pltpu.roll(v, 1, 1) for v in f])
            f = face(here, [pltpu.roll(v, ny - 1, 0) for v in here], wy)
            acc = add_here(acc, f)
            acc = add_there(acc, [pltpu.roll(v, 1, 0) for v in f])
            later = None
            if x + 1 < nx:
                here, old = plane(x + 1), here
                f = face(old, here)
                acc = add_here(acc, f)
                later = turn(f)
            for q in range(9):
                accs[q][x * ny : (x + 1) * ny, :] = acc[q]
            acc = later

    def sweeps(fresh, own, tiles_x, tiles_y, base, ext, cext):
        odd_x, odd_y, _ = place_of()
        grids = [(ext, 0), (ext, ex), (cext, 0)]
        ext[...] = jnp.zeros_like(ext)
        if fresh:
            cext[...] = jnp.zeros_like(cext)
        past = base[0] + wide[fresh] * cy
        off_x, off_y = base[0], base[1]
        gone = 0
        for f, depth in enumerate(deep[fresh]):
            (ref, row), (grid, g) = own[f], grids[f]
            for x in range(cx):
                grid[g + W + x, W : W + cy, :] = ref[row + x * cy : row + (x + 1) * cy, :]
            for sy in (0, 1):
                to = W + cy if sy else W - depth
                for x in range(cx):
                    tile = pick(
                        odd_y, sy, [r[pl.ds(off_y + x, depth, stride=cx), :] for r in tiles_y]
                    )
                    grid[g + W + x, to : to + depth, :] = tile
            for sx in (0, 1):
                to = W + cx if sx else W - depth
                tile = pick(odd_x, sx, [r[off_x : off_x + depth * cy, :] for r in tiles_x])
                for i in range(depth):
                    grid[g + to + i, W : W + cy, :] = tile[i * cy : (i + 1) * cy]
                near = depth - 1
                for i in range(near):
                    x = i if sx else cx - near + i
                    at = W + cx + i if sx else W - near + i
                    for sy in (0, 1):
                        skip = 0 if sy else depth - near
                        along = [
                            pick(
                                odd_y,
                                sy,
                                [
                                    r[
                                        pl.ds(
                                            past + b * wide[fresh] * cx + gone + skip * cx + x,
                                            near,
                                            stride=cx,
                                        ),
                                        :,
                                    ]
                                    for b in range(uy)
                                ],
                            )
                            for r in tiles_x
                        ]
                        to_y = W + cy if sy else W - near
                        grid[g + at, to_y : to_y + near, :] = pick(odd_x, sx, along)
            off_x += depth * cy
            off_y += depth * cx
            gone += depth * cx
        lane = iota((ey, nz), 1)
        has_low, has_high = lane >= R, lane < nz - R
        src = [ext[x] for x in range(ex)]
        tem = [ext[ex + x] for x in range(ex)]
        con = [cext[x] for x in range(ex)]
        inv = [1.0 / (SINK + 6.0 * c) for c in con]
        for s in range(1, W + 1):
            new = list(tem)
            for x in range(s, ex - s):
                t = tem[x]
                total = tem[x - 1] + tem[x + 1]
                total = total + (pltpu.roll(t, 1, 0) + pltpu.roll(t, ey - 1, 0))
                total = total + jnp.where(has_low, pltpu.roll(t, R, 1), 0.0)
                total = total + jnp.where(has_high, pltpu.roll(t, nz - R, 1), 0.0)
                new[x] = (src[x] + con[x] * total) * inv[x]
            tem = new
        return [tem[W + x][W : W + cy, :] for x in range(cx)]

    def outer_kernel(k, split):
        first, fresh = k == 0, k == 1

        def kernel(state, eps, ele, dop, cond, *rest):
            rest = list(rest)
            take = lambda c: [rest.pop(0) for _ in range(c)]
            accs = take(9)
            got0 = take(ux + uy)
            got = got0 if first else take(ux + uy)
            (tile,) = take(1)
            cext = None if first or fresh else take(1)[0]
            if not split:
                out, *faces = take(1 + ux)
            sends = take(uy)
            (tile_out,) = take(1)
            if fresh:
                (cext,) = take(1)
            rim_x, rim_y, temp, heat, ext, mobs = take(6)
            odd_x, odd_y, weights = place_of()

            if first:
                temp[...] = tile[...]
            else:
                own = [(tile, 0), (tile, cells), (cond, 0)]
                rows = sweeps(fresh, own, got[:ux], got[ux:], (3 * ny, 3 * nx), ext, cext)
                for x in range(cx):
                    temp[x * cy : (x + 1) * cy, :] = rows[x]
            mobs[...] = 1.0 / (1.0 + DROP * temp[...])

            def side(axis, which, f):
                src = got0 if f == 3 else got
                if axis == 0:
                    return pick(odd_x, which, [r[f * ny : (f + 1) * ny, :] for r in src[:ux]])
                return pick(odd_y, which, [r[f * nx : (f + 1) * nx, :] for r in src[ux:]])

            def edge(rows):
                return [state[f, rows, :] for f in range(3)] + [eps[3, rows, :]]

            at = [
                (0, 0, slice(0, ny)), (0, 1, slice(nodes - ny, nodes)),
                (1, 0, pl.ds(0, nx, stride=ny)), (1, 1, pl.ds(ny - 1, nx, stride=ny)),
            ]
            for axis, which, rows in at:
                there = [side(axis, which, f) for f in range(4)]
                here = edge(rows)
                weight = weights[2 * axis + which]
                f = face(here, there, weight) if which else turn(face(there, here, weight))
                for q, v in enumerate(f):
                    (rim_y if axis else rim_x)[9 * which + q] = v

            hsum = None
            for x in range(nx):
                rows = slice(x * ny, (x + 1) * ny)
                if split:
                    (h,) = whole(accs, rim_x, rim_y, x, [8])
                    h = h / (state[1, rows, :] + state[2, rows, :])
                else:
                    if x % R == 0:
                        mob = spread_rows(mobs, (x // R) * cy, cy)
                        dopx = spread_rows(dop, (x // R) * cy, cy)
                    here = [state[0, rows, :], state[1, rows, :], state[2, rows, :], None]
                    acc = whole(accs, rim_x, rim_y, x, range(9))
                    psi, n, p, h = solve(here, acc, ele[rows, :] == 1, dopx, mob)
                    out[0, rows, :] = psi
                    out[1, rows, :] = n
                    out[2, rows, :] = p
                hsum = h if x % R == 0 else hsum + h
                if x % R == R - 1:
                    xc = x // R
                    heat[xc * ny : (xc + 1) * ny, :] = hsum

            v = heat[pl.ds(0, cells, stride=R), :]
            for j in range(1, R):
                v = v + heat[pl.ds(j, cells, stride=R), :]
            lane = iota((cells, nz), 1)
            step = 1
            while step < R:
                v = v + jnp.where(
                    lane % (2 * step) < step, pltpu.roll(v, nz - step, 1), pltpu.roll(v, step, 1)
                )
                step *= 2
            tile_out[0:cells, :] = (GAIN * 0.5 / R**3) * mobs[...] * v
            tile_out[cells : 2 * cells, :] = temp[...]
            at = 0
            if not split:
                fields = [out.at[f] for f in range(3)]
                put_x(odd_x, fields, faces)
                put_y(odd_y, fields, sends)
                at = 3 * nx
            parts = [(tile_out, 0), (tile_out, cells), (cond, 0)]
            put_cells_y(odd_y, first, parts, sends, at)

        return kernel

    def solve_kernel(state, ele, dop, tile, *rest):
        accs, (rim_x, rim_y, out, token, mobs) = rest[:9], rest[9:]
        token[...] = jnp.zeros_like(token)
        mobs[...] = 1.0 / (1.0 + DROP * tile[cells : 2 * cells, :])
        for x in range(nx):
            rows = slice(x * ny, (x + 1) * ny)
            if x % R == 0:
                mob = spread_rows(mobs, (x // R) * cy, cy)
                dopx = spread_rows(dop, (x // R) * cy, cy)
            here = [state[0, rows, :], state[1, rows, :], state[2, rows, :], None]
            acc = whole(accs, rim_x, rim_y, x, range(8)) + [None]
            psi, n, p, _ = solve(here, acc, ele[rows, :] == 1, dopx, mob)
            out[0, rows, :] = psi
            out[1, rows, :] = n
            out[2, rows, :] = p

    def join_kernel(k, fresh, has_faces):
        def kernel(after, cond, tile, *rest):
            faces, got_y, s = rest[:-1][: -uy or None], rest[-1 - uy : -1], rest[-1]
            odd_x, _, _ = place_of()
            at = base = 0
            if has_faces:
                at, base = 3 * ny, 3 * nx
                s[0:at, :] = faces[0][...]
            parts = [(tile, 0), (tile, cells), (cond, 0)]
            at = put_cells_x(odd_x == (k == 0), fresh, parts, [s], at)
            more = wide[fresh] * cx
            for b in range(uy):
                s[at + b * more : at + (b + 1) * more, :] = got_y[b][base : base + more, :]

        return kernel

    def join(after, cond, tile, faces, got_y, fresh):
        sends = []
        rows = (3 * ny if faces else 0) + wide[fresh] * (cy + cx * uy)
        for k in range(ux)[::-1]:
            (after,) = call(
                join_kernel(k, fresh, bool(faces)), [(rows, nz)], [],
                [after, cond, tile] + faces[k : k + 1] + got_y, nodes,
            )
            sends.insert(0, after)
        return sends

    def final_kernel(cext, *rest):
        got, (tile, out, ext, flat) = rest[: ux + uy], rest[ux + uy :]
        own = [(tile, 0), (tile, cells)]
        rows = sweeps(False, own, got[:ux], got[ux:], (0, 0), ext, cext)
        for x in range(cx):
            flat[x * cy : (x + 1) * cy, :] = rows[x]
        coarse = nz // R
        sel = (iota((nz, coarse), 0) == R * iota((nz, coarse), 1)).astype(F32)
        out[...] = jnp.dot(
            flat[...], sel, precision=lax.Precision.HIGHEST, preferred_element_type=F32
        )

    def along(axis, pairings, sends):
        return [lax.ppermute(s, axis, pairs) for s, pairs in zip(sends, pairings)]

    def across(sends):
        got = []
        for k, pairs in enumerate(px):
            got.append(lax.ppermute(sends[k], "gx", pairs))
        return got

    def per_device(sol, ins, ele, zone, cat, warm):
        ele = ele.reshape(nodes, nz)
        coarse = nz // R
        work = nodes * nz
        V = pltpu.VMEM
        marks = lax.broadcast_in_dim(ins, (1, nx, ny, nz), (1, 2, 3))
        marks = lax.pad(marks, jnp.int32(-1), [(3, 0, 0)] + [(0, 0, 0)] * 3)
        sol = lax.pad(sol, F32(0), [(0, 1, 0)] + [(0, 0, 0)] * 3)
        start = jnp.where(marks < 0, sol, jnp.where(marks == 1, 0.4, 1.0).astype(F32))
        state = eps = start.reshape(4, nodes, nz)
        sends = call(
            pack_kernel, [(4 * ny, nz)] * ux + [(4 * nx, nz)] * uy, [], [state], work
        )
        dop, cond, tile = call(
            table_kernel, [(cells, nz)] * 3, [],
            [sends[0], zone.reshape(cells, coarse), cat.reshape(cells, coarse),
             warm.reshape(cells, coarse)],
            work,
        )
        got0 = along("gx", px, sends[:ux]) + along("gy", py, sends[ux:])
        got_y, faces, cext = [], [], []
        for k in range(NEWTON):
            first, fresh, last = k == 0, k == 1, k == NEWTON - 1
            accs = call(inner_kernel, [(nodes, nz)] * 9, [], [state, eps], 200 * work)
            got = []
            if not first:
                joined = join(accs[0], cond, tile, faces, got_y, fresh)
                got = across(joined) + got_y
            args = [state, eps, ele, dop, cond] + accs + got0 + got + [tile]
            outs = []
            if not (first or fresh):
                args += cext
            if not last:
                outs += [(3, nodes, nz)] + [(3 * ny, nz)] * ux
            outs += [((0 if last else 3 * nx) + wide[first] * cx, nz)] * uy
            outs += [(2 * cells, nz)]
            if fresh:
                outs += [(ex, ey, nz)]
            rims = [(18, ny, nz), (18, nx, nz)]
            scratch = [
                V((cells, nz), F32), V((cx * ny, nz), F32), V((2 * ex, ey, nz), F32),
                V((cells, nz), F32),
            ]
            if last:
                outs += rims
            else:
                scratch = [V(r, F32) for r in rims] + scratch
            res = call(outer_kernel(k, last), outs, scratch, args, 100 * work)
            take = lambda c: [res.pop(0) for _ in range(c)]
            if not last:
                state, *faces = take(1 + ux)
            got_y = along("gy", py, take(uy))
            (tile,) = take(1)
            if fresh:
                cext = take(1)
            if last:
                state, token = call(
                    solve_kernel, [(3, nodes, nz), (8, nz)], [V((cells, nz), F32)],
                    [state, ele, dop, tile] + accs + res, 100 * work,
                )
        joined = join(token, cond, tile, [], got_y, False)
        got = across(joined) + got_y
        (warm,) = call(
            final_kernel,
            [(cells, coarse)],
            [V((2 * ex, ey, nz), F32), V((cells, nz), F32)],
            cext + got + [tile],
            work,
        )
        return state.reshape(3, nx, ny, nz), warm.reshape(cx, cy, coarse)

    return per_device


def solution(mesh):
    placed = (
        P(None, "gx", "gy", None),
        P("gx", "gy", None),
        P("gx", "gy", None),
        P("gx", "gy", None),
        P("gx", "gy", None),
        P("gx", "gy", None),
    )
    gx, gy = mesh.shape["gx"], mesh.shape["gy"]

    def body(sol, *rest):
        _, nx, ny, nz = sol.shape
        return make(nx, ny, nz, gx, gy)(sol, *rest)

    return jax.shard_map(
        body,
        mesh=mesh,
        in_specs=placed,
        out_specs=(P(None, "gx", "gy", None), P("gx", "gy", None)),
        check_vma=False,
    )
```

```python
import jax
import jax.numpy as jnp
from jax import lax
from jax.experimental import pallas as pl
from jax.experimental.pallas import tpu as pltpu
from jax.sharding import PartitionSpec as P


R = 4
NEWTON = 3
SWEEPS = 3

POISSON = 2.0
CHARGE = 4.0
SHIFT = 24.0
BIAS = 0.25
GAIN = 1.0
SINK = 0.3
DROP = 0.5
DOPING = (-2.0, -0.5, 0.5, 2.0)
CONDUCT = (0.5, 1.0, 2.0, 4.0)

F32 = jnp.float32


def phases(count):
    out = []
    for start in (0, 1):
        pairs = []
        for i in range(start, count - 1, 2):
            pairs += [(i, i + 1), (i + 1, i)]
        if pairs:
            out.append(pairs)
    return out


def lookup(labels, table):
    value = jnp.full(labels.shape, table[0], F32)
    for level in range(1, len(table)):
        value = jnp.where(labels == level, table[level], value)
    return value


def face(here, there, weight=None):
    psi_i, n_i, p_i, e_i = here
    psi_j, n_j, p_j, e_j = there
    d = psi_j - psi_i
    small = jnp.abs(d) < 0.25
    r = 1.0 / jnp.where(small, 1.0, jnp.exp(d) - 1.0)
    q = d * d
    b = jnp.where(
        small, (1.0 - 0.5 * d) + q * (1 / 12 - q * (1 / 720 - q * (1 / 30240))), d * r
    )
    bm = b + d
    s = jnp.where(small, -0.5 + d * (1 / 6 - q * (1 / 180 - q * (1 / 5040))), r * (1.0 - bm))
    e = 0.5 * (e_i + e_j)
    if weight is None:
        gn = n_i + (n_i - n_j) * s
        gp = (p_i - p_j) * s - p_j
    else:
        b = b * weight
        bm = b + d * weight
        s = s * weight
        e = e * weight
        gn = n_i * weight + (n_i - n_j) * s
        gp = (p_i - p_j) * s - p_j * weight
    fe = n_j * b - n_i * bm
    fh = p_j * bm - p_i * b
    j = fe - fh
    return e * d, e, fe, fh, gn, gp, b, bm, j * j


def add_here(acc, f):
    lap, es, fe, fh, gn, gp, b, bm, h = f
    return [x + y for x, y in zip(acc, (lap, es, fe, fh, gn, gp, b, bm, h))]


def add_there(acc, f):
    lap, es, fe, fh, gn, gp, b, bm, h = f
    return [
        acc[0] - lap, acc[1] + es, acc[2] - fe, acc[3] - fh,
        acc[4] + gn, acc[5] + gp, acc[6] + bm, acc[7] + b, acc[8] + h,
    ]


def ahead(psi, n, p):
    total = n + p
    rden = 1.0 / (total + 2.0)
    rn = (p + 1.0) * rden
    rp = (n + 1.0) * rden
    return (n * p - 1.0) * rden, rn * rn, rp * rp, 1.0 / total, 1.0 / n, 1.0 / p


def solve(here, acc, pre, contact, dop, mob):
    psi, n, p = here
    lap, es, fe, fh, gn, gp, fwd, bwd, h = acc
    rec, rn, rp, over_total, over_n, over_p = pre
    r0 = POISSON * lap + CHARGE * (p - n + dop)
    r1 = mob * fe - rec
    r2 = mob * fh - rec
    a = -POISSON * es
    b1 = mob * gn
    b2 = -mob * bwd - rn - SHIFT
    g1 = mob * gp
    g3 = -mob * fwd - rp - SHIFT
    caa = b2 * g3 - rp * rn
    cab = -(rp * g1 + b1 * g3)
    cac = -(b1 * rn + b2 * g1)
    rdet = 1.0 / (a * caa + CHARGE * (cac - cab))
    cb1 = CHARGE * b1
    cg1 = CHARGE * g1
    s0 = (caa * r0 + CHARGE * ((g3 - rn) * r1 + (rp - b2) * r2)) * rdet
    s1 = (cab * r0 + (a * g3 - cg1) * r1 + (cb1 + a * rp) * r2) * rdet
    s2 = (cac * r0 + (a * rn - cg1) * r1 + (a * b2 + cb1) * r2) * rdet
    s0 = jnp.where(contact, psi - BIAS * dop, s0)
    s1 = jnp.where(contact, n - 1.0, s1)
    s2 = jnp.where(contact, p - 1.0, s2)
    heat = None if h is None else h * over_total
    return psi - s0, n * jnp.exp(-s1 * over_n), p * jnp.exp(-s2 * over_p), heat


def iota(shape, axis):
    return lax.broadcasted_iota(jnp.int32, shape, axis)


def spread_rows(ref, first, count):
    lanes = ref.shape[-1]
    group = iota((count * R, lanes), 0) // R
    out = jnp.broadcast_to(ref[first : first + 1, :], (count * R, lanes))
    for j in range(1, count):
        out = jnp.where(group == j, ref[first + j : first + j + 1, :], out)
    return out


def make(nx, ny, nz, gx, gy):
    cx, cy = nx // R, ny // R
    cells = cx * cy
    W = SWEEPS
    px, py = phases(gx), phases(gy)
    ux, uy = len(px), len(py)
    ex, ey = cx + 2 * W, -(-(cy + 2 * W) // 8) * 8
    nodes = nx * ny
    params = pltpu.CompilerParams(vmem_limit_bytes=16 * 1024 * 1024)
    vmem = pl.BlockSpec(memory_space=pltpu.VMEM)
    deep = {True: (W - 1, W, W - 1), False: (W - 1, W)}
    wide = {f: sum(deep[f]) for f in deep}
    corner = {f: sum((d - 1) ** 2 for d in deep[f]) for f in deep}

    def call(kernel, outs, scratch, args, cost):
        return list(
            pl.pallas_call(
                kernel,
                out_shape=[jax.ShapeDtypeStruct(s, F32) for s in outs],
                in_specs=[vmem] * len(args),
                out_specs=[vmem] * len(outs),
                scratch_shapes=scratch,
                compiler_params=params,
                cost_estimate=pl.CostEstimate(flops=cost, bytes_accessed=0, transcendentals=0),
            )(*args)
        )

    def place_of():
        ix, iy = lax.axis_index("gx"), lax.axis_index("gy")
        some = lambda test: jnp.where(test, 1.0, 0.0)
        weights = [some(ix > 0), some(ix < gx - 1), some(iy > 0), some(iy < gy - 1)]
        return ix % 2 == 1, iy % 2 == 1, weights

    def pick(odd, which, values):
        get = lambda k: values[k] if k < len(values) else jnp.zeros_like(values[0])
        return jnp.where(odd, get(which), get(1 - which))

    def put_x(odd, fields, sends):
        for f, ref in enumerate(fields):
            low, high = ref[0:ny, :], ref[(nx - 1) * ny : nodes, :]
            for k, send in enumerate(sends):
                first, second = (low, high) if k == 0 else (high, low)
                send[f * ny : (f + 1) * ny, :] = jnp.where(odd, first, second)

    def put_y(odd, fields, sends):
        for f, ref in enumerate(fields):
            low = ref[pl.ds(0, nx, stride=ny), :]
            high = ref[pl.ds(ny - 1, nx, stride=ny), :]
            for k, send in enumerate(sends):
                first, second = (low, high) if k == 0 else (high, low)
                send[f * nx : (f + 1) * nx, :] = jnp.where(odd, first, second)

    def put_cells_y(odd, fresh, fields, sends, at):
        for (ref, base), depth in zip(fields, deep[fresh]):
            for i in range(depth):
                low = ref[pl.ds(base + i, cx, stride=cy), :]
                high = ref[pl.ds(base + cy - depth + i, cx, stride=cy), :]
                for k, send in enumerate(sends):
                    first, second = (low, high) if k == 0 else (high, low)
                    send[at : at + cx, :] = jnp.where(odd, first, second)
                at += cx

    def put_cells_x(odd, fresh, fields, sends, at):
        for (ref, base), depth in zip(fields, deep[fresh]):
            low = ref[base : base + depth * cy, :]
            high = ref[base + cells - depth * cy : base + cells, :]
            for k, send in enumerate(sends):
                first, second = (low, high) if k == 0 else (high, low)
                send[at : at + depth * cy, :] = jnp.where(odd, first, second)
            at += depth * cy
        return at

    def turn(f):
        lap, es, fe, fh, gn, gp, b, bm, h = f
        return [-lap, es, -fe, -fh, gn, gp, bm, b, h]

    def whole(accs, rim_x, rim_y, x, qs):
        row = iota((8, nz), 0)
        out = []
        for q in qs:
            a = accs[q][x * ny : (x + 1) * ny, :]
            if x == 0:
                a = a + rim_x[q]
            if x == nx - 1:
                a = a + rim_x[9 + q]
            parts = [a[r : r + 8] for r in range(0, ny, 8)]
            parts[0] = parts[0] + jnp.where(row == 0, rim_y[q, x : x + 1, :], 0.0)
            parts[-1] = parts[-1] + jnp.where(row == 7, rim_y[9 + q, x : x + 1, :], 0.0)
            out.append(jnp.concatenate(parts, 0) if len(parts) > 1 else parts[0])
        return out

    def pack_kernel(start, *sends):
        odd_x, odd_y, _ = place_of()
        fields = [start.at[f] for f in range(4)]
        put_x(odd_x, fields, sends[:ux])
        put_y(odd_y, fields, sends[ux:])

    def table_kernel(after, zone, cat, warm, dop, cond, temp):
        coarse = nz // R
        pickz = (iota((coarse, nz), 1) // R == iota((coarse, nz), 0)).astype(F32)

        def widen(x):
            return jnp.dot(x, pickz, precision=lax.Precision.HIGHEST, preferred_element_type=F32)

        dop[...] = widen(lookup(zone[...], DOPING))
        cond[...] = widen(lookup(cat[...], CONDUCT))
        temp[...] = widen(warm[...])

    def inner_kernel(state, eps, *accs):
        zlane = iota((ny, nz), 1)
        wz = jnp.where(zlane < nz - 1, 1.0, 0.0)
        wy = jnp.where(iota((ny, nz), 0) < ny - 1, 1.0, 0.0)

        def plane(x):
            rows = slice(x * ny, (x + 1) * ny)
            return [state[0, rows, :], state[1, rows, :], state[2, rows, :], eps[3, rows, :]]

        here = plane(0)
        acc = None
        for x in range(nx):
            for q, v in enumerate(ahead(*here[:3])):
                accs[9 + q][x * ny : (x + 1) * ny, :] = v
            f = face(here, [pltpu.roll(v, nz - 1, 1) for v in here], wz)
            acc = list(f) if acc is None else add_here(acc, f)
            acc = add_there(acc, [pltpu.roll(v, 1, 1) for v in f])
            f = face(here, [pltpu.roll(v, ny - 1, 0) for v in here], wy)
            acc = add_here(acc, f)
            acc = add_there(acc, [pltpu.roll(v, 1, 0) for v in f])
            later = None
            if x + 1 < nx:
                here, old = plane(x + 1), here
                f = face(old, here)
                acc = add_here(acc, f)
                later = turn(f)
            for q in range(9):
                accs[q][x * ny : (x + 1) * ny, :] = acc[q]
            acc = later

    def sweeps(fresh, own, tiles_x, tiles_y, base, ext, cext):
        odd_x, odd_y, _ = place_of()
        grids = [(ext, 0), (ext, ex), (cext, 0)]
        ext[...] = jnp.zeros_like(ext)
        if fresh:
            cext[...] = jnp.zeros_like(cext)
        past = base[0] + wide[fresh] * cy
        off_x, off_y = base[0], base[1]
        gone = 0
        for f, depth in enumerate(deep[fresh]):
            (ref, row), (grid, g) = own[f], grids[f]
            for x in range(cx):
                grid[g + W + x, W : W + cy, :] = ref[row + x * cy : row + (x + 1) * cy, :]
            for sy in (0, 1):
                to = W + cy if sy else W - depth
                for x in range(cx):
                    tile = pick(
                        odd_y, sy, [r[pl.ds(off_y + x, depth, stride=cx), :] for r in tiles_y]
                    )
                    grid[g + W + x, to : to + depth, :] = tile
            for sx in (0, 1):
                to = W + cx if sx else W - depth
                tile = pick(odd_x, sx, [r[off_x : off_x + depth * cy, :] for r in tiles_x])
                for i in range(depth):
                    grid[g + to + i, W : W + cy, :] = tile[i * cy : (i + 1) * cy]
                near = depth - 1
                for i in range(near):
                    at = W + cx + i if sx else W - near + i
                    for sy in (0, 1):
                        along = [
                            pick(
                                odd_y,
                                sy,
                                [
                                    r[pl.ds(past + b * corner[fresh] + gone + i, near, stride=near), :]
                                    for b in range(uy)
                                ],
                            )
                            for r in tiles_x
                        ]
                        to_y = W + cy if sy else W - near
                        grid[g + at, to_y : to_y + near, :] = pick(odd_x, sx, along)
            off_x += depth * cy
            off_y += depth * cx
            gone += near * near
        lane = iota((ey, nz), 1)
        has_low, has_high = lane >= R, lane < nz - R
        src = [ext[x] for x in range(ex)]
        tem = [ext[ex + x] for x in range(ex)]
        con = [cext[x] for x in range(ex)]
        inv = [1.0 / (SINK + 6.0 * c) for c in con]
        for s in range(1, W + 1):
            new = list(tem)
            for x in range(s, ex - s):
                t = tem[x]
                total = tem[x - 1] + tem[x + 1]
                total = total + (pltpu.roll(t, 1, 0) + pltpu.roll(t, ey - 1, 0))
                total = total + jnp.where(has_low, pltpu.roll(t, R, 1), 0.0)
                total = total + jnp.where(has_high, pltpu.roll(t, nz - R, 1), 0.0)
                new[x] = (src[x] + con[x] * total) * inv[x]
            tem = new
        return [tem[W + x][W : W + cy, :] for x in range(cx)]

    def outer_kernel(k, split):
        first, fresh = k == 0, k == 1

        def kernel(state, eps, ele, dop, cond, *rest):
            rest = list(rest)
            take = lambda c: [rest.pop(0) for _ in range(c)]
            accs = take(9)
            pre = take(6)
            got0 = take(ux + uy)
            got = got0 if first else take(ux + uy)
            (tile,) = take(1)
            cext = None if first or fresh else take(1)[0]
            if not split:
                out, *faces = take(1 + ux)
            sends = take(uy)
            (tile_out,) = take(1)
            if fresh:
                (cext,) = take(1)
            rim_x, rim_y, temp, heat, ext, mobs = take(6)
            odd_x, odd_y, weights = place_of()

            if first:
                temp[...] = tile[...]
            else:
                own = [(tile, 0), (tile, cells), (cond, 0)]
                rows = sweeps(fresh, own, got[:ux], got[ux:], (3 * ny, 3 * nx), ext, cext)
                for x in range(cx):
                    temp[x * cy : (x + 1) * cy, :] = rows[x]
            mobs[...] = 1.0 / (1.0 + DROP * temp[...])

            def side(axis, which, f):
                src = got0 if f == 3 else got
                if axis == 0:
                    return pick(odd_x, which, [r[f * ny : (f + 1) * ny, :] for r in src[:ux]])
                return pick(odd_y, which, [r[f * nx : (f + 1) * nx, :] for r in src[ux:]])

            def edge(rows):
                return [state[f, rows, :] for f in range(3)] + [eps[3, rows, :]]

            at = [
                (0, 0, slice(0, ny)), (0, 1, slice(nodes - ny, nodes)),
                (1, 0, pl.ds(0, nx, stride=ny)), (1, 1, pl.ds(ny - 1, nx, stride=ny)),
            ]
            for axis, which, rows in at:
                there = [side(axis, which, f) for f in range(4)]
                here = edge(rows)
                weight = weights[2 * axis + which]
                f = face(here, there, weight) if which else turn(face(there, here, weight))
                for q, v in enumerate(f):
                    (rim_y if axis else rim_x)[9 * which + q] = v

            hsum = None
            for x in range(nx):
                rows = slice(x * ny, (x + 1) * ny)
                if split:
                    (h,) = whole(accs, rim_x, rim_y, x, [8])
                    h = h * pre[3][rows, :]
                else:
                    if x % R == 0:
                        mob = spread_rows(mobs, (x // R) * cy, cy)
                        dopx = spread_rows(dop, (x // R) * cy, cy)
                    here = [state[f, rows, :] for f in range(3)]
                    acc = whole(accs, rim_x, rim_y, x, range(9))
                    psi, n, p, h = solve(here, acc, [v[rows, :] for v in pre], ele[rows, :] == 1, dopx, mob)
                    out[0, rows, :] = psi
                    out[1, rows, :] = n
                    out[2, rows, :] = p
                hsum = h if x % R == 0 else hsum + h
                if x % R == R - 1:
                    xc = x // R
                    heat[xc * ny : (xc + 1) * ny, :] = hsum

            v = heat[pl.ds(0, cells, stride=R), :]
            for j in range(1, R):
                v = v + heat[pl.ds(j, cells, stride=R), :]
            lane = iota((cells, nz), 1)
            step = 1
            while step < R:
                v = v + jnp.where(
                    lane % (2 * step) < step, pltpu.roll(v, nz - step, 1), pltpu.roll(v, step, 1)
                )
                step *= 2
            tile_out[0:cells, :] = (GAIN * 0.5 / R**3) * mobs[...] * v
            tile_out[cells : 2 * cells, :] = temp[...]
            at = 0
            if not split:
                fields = [out.at[f] for f in range(3)]
                put_x(odd_x, fields, faces)
                put_y(odd_y, fields, sends)
                at = 3 * nx
            parts = [(tile_out, 0), (tile_out, cells), (cond, 0)]
            put_cells_y(odd_y, first, parts, sends, at)

        return kernel

    def solve_kernel(state, ele, dop, tile, *rest):
        accs, pre, (rim_x, rim_y, out, token, mobs) = rest[:9], rest[9:15], rest[15:]
        token[...] = jnp.zeros_like(token)
        mobs[...] = 1.0 / (1.0 + DROP * tile[cells : 2 * cells, :])
        for x in range(nx):
            rows = slice(x * ny, (x + 1) * ny)
            if x % R == 0:
                mob = spread_rows(mobs, (x // R) * cy, cy)
                dopx = spread_rows(dop, (x // R) * cy, cy)
            here = [state[f, rows, :] for f in range(3)]
            acc = whole(accs, rim_x, rim_y, x, range(8)) + [None]
            psi, n, p, _ = solve(here, acc, [v[rows, :] for v in pre], ele[rows, :] == 1, dopx, mob)
            out[0, rows, :] = psi
            out[1, rows, :] = n
            out[2, rows, :] = p

    def join_kernel(k, fresh, has_faces):
        def kernel(after, cond, tile, *rest):
            faces, got_y, s = rest[:-1][: -uy or None], rest[-1 - uy : -1], rest[-1]
            odd_x, odd_y, _ = place_of()
            to_low = odd_x == (k == 0)
            at = base = 0
            if has_faces:
                at, base = 3 * ny, 3 * nx
                s[0:at, :] = faces[0][...]
            parts = [(tile, 0), (tile, cells), (cond, 0)]
            at = put_cells_x(to_low, fresh, parts, [s], at)
            for b, g in enumerate(got_y):
                from_high = odd_y == (b == 1)
                off = base
                for depth in deep[fresh]:
                    near = depth - 1
                    for i in range(near):
                        ends = []
                        for layer in (i, depth - near + i):
                            row = off + layer * cx
                            low, high = g[row : row + near, :], g[row + cx - near : row + cx, :]
                            ends.append(jnp.where(to_low, low, high))
                        s[at : at + near, :] = jnp.where(from_high, *ends)
                        at += near
                    off += depth * cx

        return kernel

    def join(after, cond, tile, faces, got_y, fresh):
        sends = []
        rows = (3 * ny if faces else 0) + wide[fresh] * cy + corner[fresh] * uy
        for k in range(ux)[::-1]:
            (after,) = call(
                join_kernel(k, fresh, bool(faces)), [(rows, nz)], [],
                [after, cond, tile] + faces[k : k + 1] + got_y, nodes,
            )
            sends.insert(0, after)
        return sends

    def final_kernel(cext, *rest):
        got, (tile, out, ext, flat) = rest[: ux + uy], rest[ux + uy :]
        own = [(tile, 0), (tile, cells)]
        rows = sweeps(False, own, got[:ux], got[ux:], (0, 0), ext, cext)
        for x in range(cx):
            flat[x * cy : (x + 1) * cy, :] = rows[x]
        first = jnp.minimum(R * iota((cells, nz), 1), nz - 1)
        out[...] = jnp.take_along_axis(flat[...], first, axis=1)[:, : nz // R]

    def along(axis, pairings, sends):
        return [lax.ppermute(s, axis, pairs) for s, pairs in zip(sends, pairings)]

    def across(sends):
        got = []
        for k, pairs in enumerate(px):
            got.append(lax.ppermute(sends[k], "gx", pairs))
        return got

    def per_device(sol, ins, ele, zone, cat, warm):
        ele = ele.reshape(nodes, nz)
        coarse = nz // R
        work = nodes * nz
        V = pltpu.VMEM
        marks = lax.broadcast_in_dim(ins, (1, nx, ny, nz), (1, 2, 3))
        marks = lax.pad(marks, jnp.int32(-1), [(3, 0, 0)] + [(0, 0, 0)] * 3)
        sol = lax.pad(sol, F32(0), [(0, 1, 0)] + [(0, 0, 0)] * 3)
        start = jnp.where(marks < 0, sol, jnp.where(marks == 1, 0.4, 1.0).astype(F32))
        state = eps = start.reshape(4, nodes, nz)
        sends = call(
            pack_kernel, [(4 * ny, nz)] * ux + [(4 * nx, nz)] * uy, [], [state], work
        )
        dop, cond, tile = call(
            table_kernel, [(cells, nz)] * 3, [],
            [sends[0], zone.reshape(cells, coarse), cat.reshape(cells, coarse),
             warm.reshape(cells, coarse)],
            work,
        )
        got0 = along("gx", px, sends[:ux]) + along("gy", py, sends[ux:])
        got_y, faces, cext = [], [], []
        for k in range(NEWTON):
            first, fresh, last = k == 0, k == 1, k == NEWTON - 1
            accs = call(inner_kernel, [(nodes, nz)] * 15, [], [state, eps], 200 * work)
            got = []
            if not first:
                joined = join(accs[0], cond, tile, faces, got_y, fresh)
                got = across(joined) + got_y
            args = [state, eps, ele, dop, cond] + accs + got0 + got + [tile]
            outs = []
            if not (first or fresh):
                args += cext
            if not last:
                outs += [(3, nodes, nz)] + [(3 * ny, nz)] * ux
            outs += [((0 if last else 3 * nx) + wide[first] * cx, nz)] * uy
            outs += [(2 * cells, nz)]
            if fresh:
                outs += [(ex, ey, nz)]
            rims = [(18, ny, nz), (18, nx, nz)]
            scratch = [
                V((cells, nz), F32), V((cx * ny, nz), F32), V((2 * ex, ey, nz), F32),
                V((cells, nz), F32),
            ]
            if last:
                outs += rims
            else:
                scratch = [V(r, F32) for r in rims] + scratch
            res = call(outer_kernel(k, last), outs, scratch, args, 100 * work)
            take = lambda c: [res.pop(0) for _ in range(c)]
            if not last:
                state, *faces = take(1 + ux)
            got_y = along("gy", py, take(uy))
            (tile,) = take(1)
            if fresh:
                cext = take(1)
            if last:
                state, token = call(
                    solve_kernel, [(3, nodes, nz), (8, nz)], [V((cells, nz), F32)],
                    [state, ele, dop, tile] + accs + res, 100 * work,
                )
        joined = join(token, cond, tile, [], got_y, False)
        got = across(joined) + got_y
        (warm,) = call(
            final_kernel,
            [(cells, coarse)],
            [V((2 * ex, ey, nz), F32), V((cells, nz), F32)],
            cext + got + [tile],
            work,
        )
        return state.reshape(3, nx, ny, nz), warm.reshape(cx, cy, coarse)

    return per_device


def solution(mesh):
    placed = (
        P(None, "gx", "gy", None),
        P("gx", "gy", None),
        P("gx", "gy", None),
        P("gx", "gy", None),
        P("gx", "gy", None),
        P("gx", "gy", None),
    )
    gx, gy = mesh.shape["gx"], mesh.shape["gy"]

    def body(sol, *rest):
        _, nx, ny, nz = sol.shape
        return make(nx, ny, nz, gx, gy)(sol, *rest)

    return jax.shard_map(
        body,
        mesh=mesh,
        in_specs=placed,
        out_specs=(P(None, "gx", "gy", None), P("gx", "gy", None)),
        check_vma=False,
    )
```
